32 devices in a mesh: gx: 8 (over z, core), gy: 4 (over y, x).
Axes of the slice: x: 2, y: 2, z: 4, core: 2. Of those that a mesh axis runs over, the one named last changes fastest.
Arguments:
- tokens: bfloat16 [512, 4096], P('gx', 'gy'), may hold values from -6 to 6
- gate_blocks: bfloat16 [4, 8, 84, 128, 128], P('gy', 'gx'), may hold values from -0.125 to 0.125
- up_blocks: bfloat16 [4, 8, 84, 128, 128], P('gy', 'gx'), may hold values from -0.125 to 0.125
- gate_coords: int32 [4, 8, 84, 2], P('gy', 'gx'), may hold values from 0 to 13, as said below
- gate_count: int32 [4, 8], P('gy', 'gx'), may hold values from 28 to 84, as said below
- down_blocks: bfloat16 [8, 4, 48, 128, 128], P('gx', 'gy'), may hold values from -0.09375 to 0.09375
- down_rows: int32 [8, 4, 8], P('gx'), may hold values from 0 to 13, as said below
- down_coords: int32 [8, 4, 48, 2], P('gx', 'gy'), may hold values from 0 to 7, as said below
- down_count: int32 [8, 4], P('gx', 'gy'), may hold values from 16 to 48, as said below
Outputs:
- mixed: bfloat16 [512, 4096], P('gx', 'gy')
The draws below stay inside these ranges and needn't reach their ends.
Inputs may be any that keep to these rules, and one draw needn't show every extreme that they name: `gate_coords`: within each tile the 84 (model-width block, hidden block) pairs are distinct, the first below 8, the second below 14; only the first gate_count slots are live. `gate_count`: some tile has all 84 slots live. `down_rows`: within each down tile the 8 hidden blocks are distinct. `down_coords`: within each down tile the 48 (kept-row index below 8, model-width block below 8) pairs are distinct; only the first down_count slots are live. `down_count`: some tile has all 48 slots live.
All inputs are finite; a program needn't handle non-finite values.
Results may differ from the reference program's by a relative error of at most 0.025.
Values may be sent and summed in bfloat16 or wider, within the bound.
A program may use at most 64 MiB of HBM per device.

```python
import jax
import jax.numpy as jnp
from jax import lax

D = 4096
FF = 14336
BLOCK = 128
TOKENS = 512
DB = 8
FB = 14
CAP = 84
LOW = 28
USED = 8
CAPD = 48
LOWD = 16
N_GX = 8
N_GY = 4


def tile_pairs(key, tiles, positions, slots, inner):
    tile_keys = jax.random.split(key, tiles)
    orders = jax.vmap(lambda one_key: jax.random.permutation(one_key, positions))(tile_keys)[:, :slots]
    return jnp.stack([orders // inner, orders % inner], -1).astype(jnp.int32)


def tile_counts(key, tiles, lowest, highest):
    counts = jax.random.randint(key, (tiles,), lowest, highest + 1)
    chosen = jax.random.randint(jax.random.fold_in(key, 7), (), 0, tiles)
    return jnp.where(jnp.arange(tiles) == chosen, highest, counts).astype(jnp.int32)


def draw_gate_coords(key, part):
    pairs = tile_pairs(jax.random.fold_in(key, 11), N_GY * N_GX, DB * FB, CAP, FB)
    return pairs.reshape(N_GY, N_GX, CAP, 2)


def draw_gate_count(key, part):
    return tile_counts(jax.random.fold_in(key, 12), N_GY * N_GX, LOW, CAP).reshape(N_GY, N_GX)


def draw_down_rows(key, part):
    tile_keys = jax.random.split(jax.random.fold_in(key, 13), N_GX * N_GY)
    orders = jax.vmap(lambda one_key: jax.random.permutation(one_key, FB))(tile_keys)[:, :USED]
    return orders.astype(jnp.int32).reshape(N_GX, N_GY, USED)


def draw_down_coords(key, part):
    pairs = tile_pairs(jax.random.fold_in(key, 14), N_GX * N_GY, USED * DB, CAPD, DB)
    return pairs.reshape(N_GX, N_GY, CAPD, 2)


def draw_down_count(key, part):
    return tile_counts(jax.random.fold_in(key, 15), N_GX * N_GY, LOWD, CAPD).reshape(N_GX, N_GY)


def shard_levels(rng, shape, cuts, least, high):
    gain, own = 1.0, jax.random.fold_in(rng, 6)
    for dim, shards_of in cuts:
        steps = jnp.exp(jax.random.uniform(jax.random.fold_in(own, dim), (shards_of,), jnp.float32, least / len(cuts), high / len(cuts)))
        gain = gain * jnp.repeat(steps, shape[dim] // shards_of).reshape([-1 if axis == dim else 1 for axis in range(len(shape))])
    return gain


def centred(own_key, extent, scale, limit, cuts=(), held_as=jnp.bfloat16):
    gain = shard_levels(own_key, extent, cuts, -0.22, 0.18) if cuts else 1.0
    values = jax.random.normal(own_key, extent, jnp.float32) * scale * gain
    return jnp.minimum(jnp.maximum(values, -limit), limit).astype(held_as)


def setup_inputs(seed: int = 0) -> dict:
    arg_keys = jax.random.split(jax.random.key(seed), 10)
    tokens = centred(arg_keys[0], (TOKENS, D), 1.0, 6.0, ((0, 8), (1, 4)))
    gate_blocks = centred(arg_keys[1], (N_GY, N_GX, CAP, BLOCK, BLOCK), (D // 2) ** -0.5, 0.125, ((0, 4), (1, 8)))
    up_blocks = centred(arg_keys[2], (N_GY, N_GX, CAP, BLOCK, BLOCK), (D // 2) ** -0.5, 0.125, ((0, 4), (1, 8)))
    gate_coords = draw_gate_coords(jax.random.fold_in(arg_keys[9], 71), 0)
    gate_count = draw_gate_count(jax.random.fold_in(arg_keys[9], 71), 0)
    down_blocks = centred(arg_keys[5], (N_GX, N_GY, CAPD, BLOCK, BLOCK), (FF * 2 // 7) ** -0.5, 0.09375, ((0, 8), (1, 4)))
    down_rows = draw_down_rows(jax.random.fold_in(arg_keys[9], 71), 0)
    down_coords = draw_down_coords(jax.random.fold_in(arg_keys[9], 71), 0)
    down_count = draw_down_count(jax.random.fold_in(arg_keys[9], 71), 0)
    return dict(tokens=tokens, gate_blocks=gate_blocks, up_blocks=up_blocks, gate_coords=gate_coords, gate_count=gate_count, down_blocks=down_blocks, down_rows=down_rows, down_coords=down_coords, down_count=down_count)


def dense_matrix(blocks, local_rows, local_cols, counts, per_row, per_col, row_blocks, col_blocks):
    tiles_a, tiles_b, slots = blocks.shape[0], blocks.shape[1], blocks.shape[2]
    live_slots = jnp.arange(slots, dtype=jnp.int32)[None, None, :] < counts[:, :, None]
    global_rows = jnp.arange(tiles_a, dtype=jnp.int32)[:, None, None] * per_row + local_rows
    global_cols = jnp.arange(tiles_b, dtype=jnp.int32)[None, :, None] * per_col + local_cols
    values = jnp.where(live_slots[..., None, None], blocks, jnp.zeros((), blocks.dtype))
    grid = jnp.zeros((row_blocks, col_blocks, BLOCK, BLOCK), blocks.dtype)
    grid = grid.at[global_rows, global_cols].add(values)
    return grid.transpose(0, 2, 1, 3).reshape(row_blocks * BLOCK, col_blocks * BLOCK)


def rounded_sum(total, term):
    held = lax.optimization_barrier(term.astype(jnp.bfloat16))
    return total + held.astype(jnp.float32)


def reference(tokens, gate_blocks, up_blocks, gate_coords, gate_count, down_blocks, down_rows, down_coords, down_count):
    model_blocks = D // BLOCK
    hidden_blocks = FF // BLOCK
    gate_weight = dense_matrix(gate_blocks, gate_coords[..., 0], gate_coords[..., 1], gate_count, DB, FB, model_blocks, hidden_blocks)
    up_weight = dense_matrix(up_blocks, gate_coords[..., 0], gate_coords[..., 1], gate_count, DB, FB, model_blocks, hidden_blocks)
    kept_rows = jnp.take_along_axis(down_rows, down_coords[..., 0], axis=2)
    down_weight = dense_matrix(down_blocks, kept_rows, down_coords[..., 1], down_count, FB, DB, hidden_blocks, model_blocks)
    gate_total = jnp.zeros((TOKENS, FF), jnp.float32)
    up_total = jnp.zeros((TOKENS, FF), jnp.float32)
    width = DB * BLOCK
    for tile_row in range(N_GY):
        columns = tokens[:, tile_row * width:(tile_row + 1) * width]
        gate_total = rounded_sum(gate_total, jnp.dot(columns, gate_weight[tile_row * width:(tile_row + 1) * width], preferred_element_type=jnp.float32))
        up_total = rounded_sum(up_total, jnp.dot(columns, up_weight[tile_row * width:(tile_row + 1) * width], preferred_element_type=jnp.float32))
    hidden = (jax.nn.silu(gate_total) * up_total).astype(jnp.bfloat16)
    out_total = jnp.zeros((TOKENS, D), jnp.float32)
    span = FB * BLOCK
    for tile_col in range(N_GX):
        part_hidden = hidden[:, tile_col * span:(tile_col + 1) * span]
        out_total = rounded_sum(out_total, jnp.dot(part_hidden, down_weight[tile_col * span:(tile_col + 1) * span], preferred_element_type=jnp.float32))
    return out_total.astype(jnp.bfloat16)
```

```python
import functools

import jax
import jax.numpy as jnp
from jax import lax
from jax.experimental import pallas as pl
from jax.experimental.pallas import tpu as pltpu
from jax.sharding import PartitionSpec as P

BLOCK = 128
LANES = 128
FF = 14336
MESH = pl.DeviceIdType.MESH
F32, BF16, I32 = jnp.float32, jnp.bfloat16, jnp.int32


def factor(n):
    low = 1
    while low * low * 4 <= n and n % (low * 2) == 0:
        low *= 2
    return n // low, low


def kernel(cfg, gco_h, gct_h, dco_h, dct_h, kept_h, tok, gblk, ublk, dblk, out,
           gco, gct, dco, dct, kept, tabv, tabs,
           gw, uw, dw, gat, pa, pb,
           r1a, r1b, s2a, s2b, r2a, r2b, acca, accb, hid, a2s, a2r, ps, fp, f2, fr, facc,
           lsem, gs, gr, s1as, s1ar, s1bs, s1br, s2as, s2ar, s2bs, s2br, xs, xr, fs, fq, fps, fpr):
    (n_gx, n_gy, n_hi, n_lo, per, nc, halves, rp, hr, n_model, fb, ca,
     cap, used, capd) = cfg
    gx, gy = lax.axis_index("gx"), lax.axis_index("gy")
    zc, mc = gx // per, gx % per
    hi, lo = gy // n_lo, gy % n_lo
    tall = per * hr
    down_at = -(-n_model * fb // LANES)

    barrier = pltpu.get_barrier_semaphore()

    def greet(dev):
        pl.semaphore_signal(barrier, inc=1, device_id=dev, device_id_type=MESH)

    for d in range(1, n_lo):
        greet((gx, hi * n_lo + (lo + d) % n_lo))
    for d in range(1, n_hi):
        greet((gx, (hi + d) % n_hi * n_lo + lo))
    for d in range(1, per):
        greet((zc * per + (mc + d) % per, gy))

    @pl.when(zc > 0)
    def _():
        greet(((zc - 1) * per + mc, gy))

    @pl.when(zc < nc - 1)
    def _():
        greet(((zc + 1) * per + mc, gy))

    smalls = [
        pltpu.make_async_copy(gco_h, gco, lsem.at[0]),
        pltpu.make_async_copy(gct_h, gct, lsem.at[1]),
        pltpu.make_async_copy(dco_h, dco, lsem.at[2]),
        pltpu.make_async_copy(dct_h, dct, lsem.at[3]),
        pltpu.make_async_copy(kept_h, kept, lsem.at[4]),
    ]
    mine = [
        pltpu.make_async_copy(tok.at[pl.ds(h * hr, hr)], gat.at[zc, h, mc], lsem.at[8 + h])
        for h in range(halves)
    ]
    loads = [
        pltpu.make_async_copy(gblk, gw.at[pl.ds(0, cap)], lsem.at[5]),
        pltpu.make_async_copy(ublk, uw.at[pl.ds(0, cap)], lsem.at[6]),
        pltpu.make_async_copy(dblk, dw.at[pl.ds(0, capd)], lsem.at[7]),
    ]
    for load in smalls + mine + loads:
        load.start()

    def table(coords, count, slots, inner, spots, first):
        wide = -(-spots // LANES)
        lane = lax.broadcasted_iota(I32, (1, LANES), 1)
        row = [jnp.full((1, LANES), slots, I32) for _ in range(wide)]
        live = count[0, 0]
        for s in range(slots):
            place = coords[0, s] * inner + coords[1, s]
            place = jnp.where(s < live, place, -1)
            for w in range(wide):
                row[w] = jnp.where(lane + w * LANES == place, s, row[w])
        for w in range(wide):
            tabv[first + w] = row[w]

    with jax.named_scope("tables"):
        for load in smalls:
            load.wait()
        table(gco, gct, cap, fb, n_model * fb, 0)
        table(dco, dct, capd, n_model, used * n_model, down_at)
        gw[cap] = jnp.zeros((BLOCK, BLOCK), BF16)
        uw[cap] = jnp.zeros((BLOCK, BLOCK), BF16)
        dw[capd] = jnp.zeros((BLOCK, BLOCK), BF16)
        tables = pltpu.make_async_copy(tabv, tabs, lsem.at[0])
        tables.start()
        for load in mine:
            load.wait()

    with jax.named_scope("barrier"):
        pl.semaphore_wait(
            barrier,
            n_lo + n_hi + per - 3 + jnp.minimum(zc, 1) + jnp.minimum(nc - 1 - zc, 1))

    sends = []

    def send(src, dst, ssem, rsem, dev, when=None):
        copy = pltpu.make_async_remote_copy(
            src_ref=src, dst_ref=dst, send_sem=ssem, recv_sem=rsem,
            device_id=dev, device_id_type=MESH)
        if when is None:
            copy.start()
        else:
            pl.when(when)(copy.start)
        sends.append((copy, when))

    def arrived(ref, sem):
        with jax.named_scope("w"):
            pltpu.make_async_remote_copy(
                src_ref=ref, dst_ref=ref, send_sem=sem, recv_sem=sem,
                device_id=(gx, (gy + 1) % n_gy), device_id_type=MESH).wait_recv()

    def share(c, h, up, down, there=None):
        def both(a, b):
            return b if a is None else a & b
        ref = gat.at[c, h, mc]
        if up:
            send(ref, ref, gs.at[c, h, 0], gr.at[c, h, mc], ((zc + 1) * per + mc, gy),
                 both(there, zc < nc - 1))
        if down:
            send(ref, ref, gs.at[c, h, 1], gr.at[c, h, mc], ((zc - 1) * per + mc, gy),
                 both(there, zc > 0))
        for j in range(1, per):
            send(ref, ref, gs.at[c, h, 1 + j], gr.at[c, h, mc],
                 (zc * per + (mc + j) % per, gy), there)

    def relay(d, h):
        for c, there, up in ((zc - d, zc >= d, True), (zc + d, zc < nc - d, False)):
            @pl.when(there)
            def _(c=c):
                arrived(gat.at[c, h, mc], gr.at[c, h, mc])

            share(c, h, up, not up, there)

    jobs = [(k, h) for k in range(nc) for h in range(halves)]
    number = {job: i for i, job in enumerate(jobs)}

    def project(job):
        j, (k, h) = number[job], job
        chip = zc ^ k
        for d in range(1, per):
            c = (mc + d) % per
            arrived(gat.at[chip, h, c], gr.at[chip, h, c])
        for part, first, many in ((pa, 0, ca), (pb, ca, fb - ca)):
            def col(c, _, part=part, first=first):
                to = pl.multiple_of(c * 2 * BLOCK, 2 * BLOCK)
                slots = []
                for r in range(n_model):
                    at = r * fb + c + first
                    slots.append(tabs[at // LANES, 0, at % LANES])
                weight = jnp.concatenate(
                    [jnp.concatenate([gw[i], uw[i]], axis=1) for i in slots], axis=0)
                y = jnp.dot(gat[chip, h].reshape(tall, n_model * BLOCK), weight,
                            preferred_element_type=F32)
                part[j, :, :, :, pl.ds(to, 2 * BLOCK)] = y.astype(BF16).reshape(
                    n_hi, n_lo, rp, 2 * BLOCK)
                return 0

            lax.fori_loop(0, many, col, 0, unroll=True)
            if part is pa:
                for d in range(1, n_lo):
                    l2 = (lo + d) % n_lo
                    send(pa.at[j, :, l2], r1a.at[j, d - 1], s1as.at[j, d - 1],
                         s1ar.at[j, d - 1], (gx, hi * n_lo + l2))
            else:
                for d in range(1, n_hi):
                    h2 = (hi + d) % n_hi
                    send(pb.at[j, h2], r1b.at[j, d - 1], s1bs.at[j, d - 1],
                         s1br.at[j, d - 1], (gx, h2 * n_lo + lo))

    def reduce(job):
        j = number[job]
        for d in range(1, n_lo):
            arrived(r1a.at[j, d - 1], s1ar.at[j, d - 1])
        for e in list(range(1, n_hi)) + [0]:
            h2 = (hi + e) % n_hi
            s = pa[j, h2, lo].astype(F32)
            for d in range(1, n_lo):
                s = s + r1a[j, d - 1, h2].astype(F32)
            if e == 0:
                acca[j] = s
            else:
                s2a[j, e - 1] = s.astype(BF16)
                send(s2a.at[j, e - 1], r2a.at[j, e - 1], s2as.at[j, e - 1],
                     s2ar.at[j, e - 1], (gx, h2 * n_lo + lo))
        for d in range(1, n_hi):
            arrived(r1b.at[j, d - 1], s1br.at[j, d - 1])
        for e in list(range(1, n_lo)) + [0]:
            l2 = (lo + e) % n_lo
            s = pb[j, hi, l2].astype(F32)
            for d in range(1, n_hi):
                s = s + r1b[j, d - 1, l2].astype(F32)
            if e == 0:
                accb[j] = s
            else:
                s2b[j, e - 1] = s.astype(BF16)
                send(s2b.at[j, e - 1], r2b.at[j, e - 1], s2bs.at[j, e - 1],
                     s2br.at[j, e - 1], (gx, hi * n_lo + l2))

    def activate(job):
        j = number[job]
        for d in range(1, n_hi):
            arrived(r2a.at[j, d - 1], s2ar.at[j, d - 1])
        for d in range(1, n_lo):
            arrived(r2b.at[j, d - 1], s2br.at[j, d - 1])
        for c in range(fb):
            acc, got, peers, at = (
                (acca, r2a, n_hi, c) if c < ca else (accb, r2b, n_lo, c - ca))
            cols = pl.ds(at * 2 * BLOCK, 2 * BLOCK)
            s = acc[j, :, cols]
            for d in range(1, peers):
                s = s + got[j, d - 1, :, cols].astype(F32)
            gate, up = s[:, :BLOCK], s[:, BLOCK:]
            hid[c] = (gate / (1.0 + jnp.exp(-gate)) * up).astype(BF16)
        others = [(a, b) for a in range(n_hi) for b in range(n_lo) if a or b]
        others.sort(key=lambda ab: -(ab[0] > 0) - (ab[1] > 0))
        for at, (a, b) in enumerate(others):
            dest = (hi + a) % n_hi * n_lo + (lo + b) % n_lo
            for q in range(used):
                a2s[j, at, :, pl.ds(q * BLOCK, BLOCK)] = hid[kept[0, dest, q]]
            send(a2s.at[j, at], a2r.at[j, gy], xs.at[j, at], xr.at[j, gy], (gx, dest))
        for q in range(used):
            a2r[j, gy, :, pl.ds(q * BLOCK, BLOCK)] = hid[kept[0, gy, q]]

    wide = 2 * BLOCK

    def mix(job):
        j = number[job]
        for d in range(1, n_gy):
            src = (gy + d) % n_gy
            arrived(a2r.at[j, src], xr.at[j, src])

        def col(c, _):
            at = pl.multiple_of(c * wide, wide)
            slots = []
            for r in range(used):
                pair = [r * n_model + c * 2 + i for i in range(2)]
                slots.append([tabs[down_at + p // LANES, 0, p % LANES] for p in pair])
            weight = jnp.concatenate(
                [jnp.concatenate([dw[i] for i in pair], axis=1) for pair in slots], axis=0)
            ps[j, :, pl.ds(at, wide)] = jnp.dot(
                a2r[j].reshape(tall, used * BLOCK), weight,
                preferred_element_type=F32).astype(BF16)
            return 0

        lax.fori_loop(0, n_model * BLOCK // wide, col, 0, unroll=True)
        for d in range(1, per):
            cj = (mc + d) % per
            send(ps.at[j, pl.ds(pl.multiple_of(cj * hr, hr), hr)], fp.at[j, d - 1],
                 fps.at[j, d - 1], fpr.at[j, d - 1], (zc * per + cj, gy))

    def finish(job):
        j, (k, h) = number[job], job
        s = ps[j, pl.ds(pl.multiple_of(mc * hr, hr), hr)].astype(F32)
        for d in range(1, per):
            arrived(fp.at[j, d - 1], fpr.at[j, d - 1])
            s = s + fp[j, d - 1].astype(F32)
        if k:
            f2[j] = s.astype(BF16)
            send(f2.at[j], fr.at[j], fs.at[j], fq.at[j], ((zc ^ k) * per + mc, gy))
        else:
            facc[h] = s

    def total(h):
        s = facc[h]
        for k in range(1, nc):
            j = number[k, h]
            arrived(fr.at[j], fq.at[j])
            s = s + fr[j].astype(F32)
        out[pl.ds(h * hr, hr)] = s.astype(BF16)

    def run(stage, *args):
        with jax.named_scope(f"{stage.__name__}#j={args}"):
            stage(*args)

    for h in range(halves):
        share(zc, h, True, True)
    tables.wait()
    with jax.named_scope("loads"):
        loads[0].wait()
        loads[1].wait()

    far = [(k, h) for k in range(1, nc) for h in range(halves)]
    far = far[:1] + [job for job in far if job[0] > 1] + [job for job in far[1:] if job[0] == 1]
    hops = [(d, h) for d in range(1, nc) for h in range(halves)]

    def need(i):
        if i < len(far):
            k, h = far[i]
            while hops and hops[0] <= (k, h):
                run(relay, *hops.pop(0))

    own = [(0, h) for h in range(halves)]
    n = len(far)
    for job in own:
        run(project, job)
    need(0)
    for i in range(n + 1):
        if i < n:
            run(project, far[i])
            need(i + 1)
        if i == 0:
            run(reduce, own[0])
            loads[2].wait()
        for lag, stage in ((1, reduce), (2, activate), (3, mix), (4, finish)):
            if 0 <= i - lag < n:
                run(stage, far[i - lag])
            if i == n and stage is activate:
                for job in own[1:]:
                    run(reduce, job)
    run(activate, far[n - 1])
    for job in own:
        run(activate, job)
    for lag in (2, 1):
        if n >= lag:
            run(mix, far[n - lag])
            if n > lag:
                run(finish, far[n - lag - 1])
    run(mix, own[0])
    run(finish, far[n - 1])
    for job in own[1:]:
        run(mix, job)
    for job in own:
        run(finish, job)
    for h in range(halves):
        run(total, h)
    for copy, when in sends:
        if when is None:
            copy.wait_send()
        else:
            pl.when(when)(copy.wait_send)


def solution(mesh):
    n_gx, n_gy = mesh.shape["gx"], mesh.shape["gy"]
    n_hi, n_lo = factor(n_gy)
    per = 2 if n_gx % 2 == 0 else 1
    nc = n_gx // per
    halves = 2

    def body(tokens, gate_blocks, up_blocks, gate_coords, gate_count,
             down_blocks, down_rows, down_coords, down_count):
        rows, width = tokens.shape
        n_model = width // BLOCK
        fb = FF // (BLOCK * n_gx)
        ca = (fb + 1) // 2
        cb = fb - ca
        cap, capd, used = gate_blocks.shape[2], down_blocks.shape[2], down_rows.shape[-1]
        hr = rows // halves
        rp = per * hr // n_gy
        jobs = nc * halves
        cfg = (n_gx, n_gy, n_hi, n_lo, per, nc, halves, rp, hr, n_model, fb, ca,
               cap, used, capd)
        wa, wb = ca * 2 * BLOCK, cb * 2 * BLOCK
        kl, kh, kg = max(n_lo - 1, 1), max(n_hi - 1, 1), max(n_gy - 1, 1)
        kp = max(per - 1, 1)
        tabs = -(-n_model * fb // LANES) + -(-used * n_model // LANES)
        vm, sm, dma = pltpu.VMEM, pltpu.SMEM, pltpu.SemaphoreType.DMA
        hbm = pl.BlockSpec(memory_space=pltpu.HBM)
        return pl.pallas_call(
            functools.partial(kernel, cfg),
            out_shape=jax.ShapeDtypeStruct((rows, width), BF16),
            in_specs=[hbm] * 9,
            out_specs=pl.BlockSpec(memory_space=pltpu.VMEM),
            scratch_shapes=[
                sm((2, cap), I32),
                sm((1, 1), I32),
                sm((2, capd), I32),
                sm((1, 1), I32),
                sm(down_rows.shape, I32),
                vm((tabs, 1, LANES), I32),
                sm((tabs, 1, LANES), I32),
                vm((cap + 1, BLOCK, BLOCK), BF16),
                vm((cap + 1, BLOCK, BLOCK), BF16),
                vm((capd + 1, BLOCK, BLOCK), BF16),
                vm((nc, halves, per, hr, width), BF16),
                vm((jobs, n_hi, n_lo, rp, wa), BF16),
                vm((jobs, n_hi, n_lo, rp, wb), BF16),
                vm((jobs, kl, n_hi, rp, wa), BF16),
                vm((jobs, kh, n_lo, rp, wb), BF16),
                vm((jobs, kh, rp, wa), BF16),
                vm((jobs, kl, rp, wb), BF16),
                vm((jobs, kh, rp, wa), BF16),
                vm((jobs, kl, rp, wb), BF16),
                vm((jobs, rp, wa), F32),
                vm((jobs, rp, wb), F32),
                vm((fb, rp, BLOCK), BF16),
                vm((jobs, kg, rp, used * BLOCK), BF16),
                vm((jobs, n_gy, rp, used * BLOCK), BF16),
                vm((jobs, per * hr, width), BF16),
                vm((jobs, kp, hr, width), BF16),
                vm((jobs, hr, width), BF16),
                vm((jobs, hr, width), BF16),
                vm((halves, hr, width), F32),
                dma((8 + halves,)),
                dma((nc, halves, 1 + per)), dma((nc, halves, per)),
                dma((jobs, kl)), dma((jobs, kl)),
                dma((jobs, kh)), dma((jobs, kh)),
                dma((jobs, kh)), dma((jobs, kh)),
                dma((jobs, kl)), dma((jobs, kl)),
                dma((jobs, kg)), dma((jobs, n_gy)),
                dma((jobs,)), dma((jobs,)),
                dma((jobs, kp)), dma((jobs, kp)),
            ],
            compiler_params=pltpu.CompilerParams(
                collective_id=0, has_side_effects=True, vmem_limit_bytes=60 * 1024 * 1024),
        )(gate_coords[0, 0].T, gate_count, down_coords[0, 0].T, down_count, down_rows,
          tokens, gate_blocks.reshape(cap, BLOCK, BLOCK),
          up_blocks.reshape(cap, BLOCK, BLOCK), down_blocks.reshape(capd, BLOCK, BLOCK))

    return jax.shard_map(
        body,
        mesh=mesh,
        in_specs=(
            P("gx", "gy"),
            P("gy", "gx", None, None, None),
            P("gy", "gx", None, None, None),
            P("gy", "gx", None, None),
            P("gy", "gx"),
            P("gx", "gy", None, None, None),
            P("gx", None, None),
            P("gx", "gy", None, None),
            P("gx", "gy"),
        ),
        out_specs=P("gx", "gy"),
        check_vma=False,
    )
```

```python
import functools

import jax
import jax.numpy as jnp
from jax import lax
from jax.experimental import pallas as pl
from jax.experimental.pallas import tpu as pltpu
from jax.sharding import PartitionSpec as P

BLOCK = 128
LANES = 128
LOADS = 1
EARLY = 1
FF = 14336
MESH = pl.DeviceIdType.MESH
F32, BF16, I32 = jnp.float32, jnp.bfloat16, jnp.int32


def factor(n):
    low = 1
    while low * low * 4 <= n and n % (low * 2) == 0:
        low *= 2
    return n // low, low


def kernel(cfg, gco_h, gct_h, dco_h, dct_h, kept_h, tok, gblk, ublk, dblk, out,
           gco, gct, dco, dct, kept, tabv, tabs,
           gw, uw, dw, gat, pa, pb,
           r1a, r1b, s2a, s2b, r2a, r2b, acca, accb, hid, a2s, a2r, ps, fp, f2, fr, facc,
           lsem, wsem, gs, gr, s1as, s1ar, s1bs, s1br, s2as, s2ar, s2bs, s2br, xs, xr, fs, fq, fps, fpr):
    (n_gx, n_gy, n_hi, n_lo, per, nc, halves, rp, hr, n_model, fb, ca,
     cap, used, capd) = cfg
    gx, gy = lax.axis_index("gx"), lax.axis_index("gy")
    zc, mc = gx // per, gx % per
    hi, lo = gy // n_lo, gy % n_lo
    tall = per * hr
    down_at = -(-n_model * fb // LANES)

    barrier = pltpu.get_barrier_semaphore()

    def greet(dev):
        pl.semaphore_signal(barrier, inc=1, device_id=dev, device_id_type=MESH)

    for d in range(1, n_lo):
        greet((gx, hi * n_lo + (lo + d) % n_lo))
    for d in range(1, n_hi):
        greet((gx, (hi + d) % n_hi * n_lo + lo))
    for d in range(1, per):
        greet((zc * per + (mc + d) % per, gy))

    @pl.when(zc > 0)
    def _():
        greet(((zc - 1) * per + mc, gy))

    @pl.when(zc < nc - 1)
    def _():
        greet(((zc + 1) * per + mc, gy))

    smalls = [
        pltpu.make_async_copy(gco_h, gco, lsem.at[0]),
        pltpu.make_async_copy(gct_h, gct, lsem.at[1]),
        pltpu.make_async_copy(dco_h, dco, lsem.at[2]),
        pltpu.make_async_copy(dct_h, dct, lsem.at[3]),
        pltpu.make_async_copy(kept_h, kept, lsem.at[4]),
    ]
    mine = [
        pltpu.make_async_copy(tok.at[pl.ds(h * hr, hr)], gat.at[zc, h, mc], lsem.at[8 + h])
        for h in range(halves)
    ]
    loads, last = [], pltpu.make_async_copy(dblk, dw.at[pl.ds(0, capd)], lsem.at[7])
    size = -(-cap // LOADS)
    for a in range(0, cap, size):
        part = pl.ds(a, min(size, cap - a))
        for i, (src, dst) in enumerate(((gblk, gw), (ublk, uw))):
            loads.append(pltpu.make_async_copy(src.at[part], dst.at[part], wsem.at[i, a // size]))
    for load in smalls + mine + loads:
        load.start()

    def table(coords, count, slots, inner, spots, first):
        wide = -(-spots // LANES)
        lane = lax.broadcasted_iota(I32, (1, LANES), 1)
        row = [jnp.full((1, LANES), slots, I32) for _ in range(wide)]
        live = count[0, 0]
        for s in range(slots):
            place = coords[0, s] * inner + coords[1, s]
            place = jnp.where(s < live, place, -1)
            for w in range(wide):
                row[w] = jnp.where(lane + w * LANES == place, s, row[w])
        for w in range(wide):
            tabv[first + w] = row[w]

    with jax.named_scope("tables"):
        for load in smalls:
            load.wait()
        table(gco, gct, cap, fb, n_model * fb, 0)
        table(dco, dct, capd, n_model, used * n_model, down_at)
        gw[cap] = jnp.zeros((BLOCK, BLOCK), BF16)
        uw[cap] = jnp.zeros((BLOCK, BLOCK), BF16)
        dw[capd] = jnp.zeros((BLOCK, BLOCK), BF16)
        tables = pltpu.make_async_copy(tabv, tabs, lsem.at[0])
        tables.start()
        for load in mine:
            load.wait()

    with jax.named_scope("barrier"):
        pl.semaphore_wait(
            barrier,
            n_lo + n_hi + per - 3 + jnp.minimum(zc, 1) + jnp.minimum(nc - 1 - zc, 1))

    sends = []

    def send(src, dst, ssem, rsem, dev, when=None):
        copy = pltpu.make_async_remote_copy(
            src_ref=src, dst_ref=dst, send_sem=ssem, recv_sem=rsem,
            device_id=dev, device_id_type=MESH)
        if when is None:
            copy.start()
        else:
            pl.when(when)(copy.start)
        sends.append((copy, when))

    def arrived(ref, sem):
        with jax.named_scope("w"):
            pltpu.make_async_remote_copy(
                src_ref=ref, dst_ref=ref, send_sem=sem, recv_sem=sem,
                device_id=(gx, (gy + 1) % n_gy), device_id_type=MESH).wait_recv()

    near = 1 - 2 * (zc % 2)

    def share(c, h, ways, there=None):
        ref = gat.at[c, h, mc]
        for at, way in enumerate(ways):
            to = zc + way
            fits = (to >= 0) & (to < nc)
            send(ref, ref, gs.at[c, h, at], gr.at[c, h, mc], (to * per + mc, gy),
                 fits if there is None else there & fits)
        for j in range(1, per):
            send(ref, ref, gs.at[c, h, 1 + j], gr.at[c, h, mc],
                 (zc * per + (mc + j) % per, gy), there)

    def relay(d, h, way):
        c = zc + way * d
        there = (c >= 0) & (c < nc)

        @pl.when(there)
        def _():
            arrived(gat.at[c, h, mc], gr.at[c, h, mc])

        share(c, h, (-way,), there)

    own = [(h, zc, h) for h in range(halves)]
    plain = [(k, h) for k in range(1, nc) for h in range(halves)]
    late = plain[:1] + [kh for kh in plain if kh[0] > 1] + plain[1:halves]
    turn = zc % 2 * jnp.minimum(nc - 1 - zc, 1)
    far = []
    for i, (a, b) in enumerate(zip(late, plain)):
        k, h = (u + turn * (v - u) if u != v else u for u, v in zip(a, b))
        far.append((halves + i, zc ^ k, h))

    def spans(many, pieces):
        size = -(-many // pieces)
        return [(a, min(a + size, many)) for a in range(0, many, size)]

    def project(first_job, count=1, pieces=1):
        j, chip, h = first_job
        for g in [h + i for i in range(count)]:
            for d in range(1, per):
                c = (mc + d) % per
                arrived(gat.at[chip, g, c], gr.at[chip, g, c])
        parts = ((pa, 0, spans(ca, pieces)), (pb, ca, spans(fb - ca, pieces)))
        for piece in range(pieces):
            for part, first, cuts in parts:
                lo_c, hi_c = cuts[piece]

                def col(i, _, part=part, first=first, lo_c=lo_c):
                    c = i + lo_c
                    to = pl.multiple_of(c * 2 * BLOCK, 2 * BLOCK)
                    slots = []
                    for r in range(n_model):
                        at = r * fb + c + first
                        slots.append(tabs[at // LANES, 0, at % LANES])
                    weight = jnp.concatenate(
                        [jnp.concatenate([gw[i], uw[i]], axis=1) for i in slots], axis=0)
                    x = gat[chip, pl.ds(h, count)].reshape(count * tall, n_model * BLOCK)
                    y = jnp.dot(x, weight, preferred_element_type=F32)
                    part[pl.ds(j, count), :, :, :, pl.ds(to, 2 * BLOCK)] = y.astype(
                        BF16).reshape(count, n_hi, n_lo, rp, 2 * BLOCK)
                    return 0

                lax.fori_loop(0, hi_c - lo_c, col, 0, unroll=True)
                cols = pl.ds(lo_c * 2 * BLOCK, (hi_c - lo_c) * 2 * BLOCK)
                for g in range(j, j + count):
                    split[g] = pieces
                    if part is pa:
                        for d in range(1, n_lo):
                            l2 = (lo + d) % n_lo
                            send(pa.at[g, :, l2, :, cols], r1a.at[g, d - 1, :, :, cols],
                                 s1as.at[g, d - 1, piece], s1ar.at[g, d - 1, piece],
                                 (gx, hi * n_lo + l2))
                    else:
                        for d in range(1, n_hi):
                            h2 = (hi + d) % n_hi
                            send(pb.at[g, h2, :, :, cols], r1b.at[g, d - 1, :, :, cols],
                                 s1bs.at[g, d - 1, piece], s1br.at[g, d - 1, piece],
                                 (gx, h2 * n_lo + lo))

    split = {}

    def first_arrived(ref, sem, many, pieces):
        for piece, (a, b) in enumerate(spans(many, pieces)):
            cols = pl.ds(a * 2 * BLOCK, (b - a) * 2 * BLOCK)
            arrived(ref.at[:, :, cols], sem.at[piece])

    def reduce(job):
        j = job[0]
        for d in range(1, n_lo):
            first_arrived(r1a.at[j, d - 1], s1ar.at[j, d - 1], ca, split[j])
        for e in list(range(1, n_hi)) + [0]:
            h2 = (hi + e) % n_hi
            s = pa[j, h2, lo].astype(F32)
            for d in range(1, n_lo):
                s = s + r1a[j, d - 1, h2].astype(F32)
            if e == 0:
                acca[j] = s
            else:
                s2a[j, e - 1] = s.astype(BF16)
                send(s2a.at[j, e - 1], r2a.at[j, e - 1], s2as.at[j, e - 1],
                     s2ar.at[j, e - 1], (gx, h2 * n_lo + lo))
        for d in range(1, n_hi):
            first_arrived(r1b.at[j, d - 1], s1br.at[j, d - 1], fb - ca, split[j])
        for e in list(range(1, n_lo)) + [0]:
            l2 = (lo + e) % n_lo
            s = pb[j, hi, l2].astype(F32)
            for d in range(1, n_hi):
                s = s + r1b[j, d - 1, l2].astype(F32)
            if e == 0:
                accb[j] = s
            else:
                s2b[j, e - 1] = s.astype(BF16)
                send(s2b.at[j, e - 1], r2b.at[j, e - 1], s2bs.at[j, e - 1],
                     s2br.at[j, e - 1], (gx, hi * n_lo + l2))

    def activate(job):
        j = job[0]
        for d in range(1, n_hi):
            arrived(r2a.at[j, d - 1], s2ar.at[j, d - 1])
        for d in range(1, n_lo):
            arrived(r2b.at[j, d - 1], s2br.at[j, d - 1])
        for c in range(fb):
            acc, got, peers, at = (
                (acca, r2a, n_hi, c) if c < ca else (accb, r2b, n_lo, c - ca))
            cols = pl.ds(at * 2 * BLOCK, 2 * BLOCK)
            s = acc[j, :, cols]
            for d in range(1, peers):
                s = s + got[j, d - 1, :, cols].astype(F32)
            gate, up = s[:, :BLOCK], s[:, BLOCK:]
            hid[c] = (gate / (1.0 + jnp.exp(-gate)) * up).astype(BF16)
        others = [(a, b) for a in range(n_hi) for b in range(n_lo) if a or b]
        others.sort(key=lambda ab: -(ab[0] > 0) - (ab[1] > 0))
        for at, (a, b) in enumerate(others):
            dest = (hi + a) % n_hi * n_lo + (lo + b) % n_lo
            for q in range(used):
                a2s[j, at, :, pl.ds(q * BLOCK, BLOCK)] = hid[kept[0, dest, q]]
            send(a2s.at[j, at], a2r.at[j, gy], xs.at[j, at], xr.at[j, gy], (gx, dest))
        for q in range(used):
            a2r[j, gy, :, pl.ds(q * BLOCK, BLOCK)] = hid[kept[0, gy, q]]

    wide = 2 * BLOCK

    def mix(job):
        j = job[0]
        for d in range(1, n_gy):
            src = (gy + d) % n_gy
            arrived(a2r.at[j, src], xr.at[j, src])

        def col(c, _):
            at = pl.multiple_of(c * wide, wide)
            slots = []
            for r in range(used):
                pair = [r * n_model + c * 2 + i for i in range(2)]
                slots.append([tabs[down_at + p // LANES, 0, p % LANES] for p in pair])
            weight = jnp.concatenate(
                [jnp.concatenate([dw[i] for i in pair], axis=1) for pair in slots], axis=0)
            ps[j, :, pl.ds(at, wide)] = jnp.dot(
                a2r[j].reshape(tall, used * BLOCK), weight,
                preferred_element_type=F32).astype(BF16)
            return 0

        lax.fori_loop(0, n_model * BLOCK // wide, col, 0, unroll=True)
        for d in range(1, per):
            cj = (mc + d) % per
            send(ps.at[j, pl.ds(pl.multiple_of(cj * hr, hr), hr)], fp.at[j, d - 1],
                 fps.at[j, d - 1], fpr.at[j, d - 1], (zc * per + cj, gy))

    def finish(job):
        j, chip, h = job
        s = ps[j, pl.ds(pl.multiple_of(mc * hr, hr), hr)].astype(F32)
        for d in range(1, per):
            arrived(fp.at[j, d - 1], fpr.at[j, d - 1])
            s = s + fp[j, d - 1].astype(F32)
        if j < halves:
            facc[j] = s
        else:
            f2[j] = s.astype(BF16)
            send(f2.at[j], fr.at[zc, h], fs.at[j], fq.at[zc, h], (chip * per + mc, gy))

    def total(h):
        s = facc[h]
        for k in range(1, nc):
            c = zc ^ k
            arrived(fr.at[c, h], fq.at[c, h])
            s = s + fr[c, h].astype(F32)
        out[pl.ds(h * hr, hr)] = s.astype(BF16)

    def run(stage, *args):
        tag = args[0][0] if isinstance(args[0], tuple) else args[0]
        with jax.named_scope(f"{stage.__name__}#j={tag}"):
            stage(*args)

    for h in range(halves):
        share(zc, h, (1, -1))
    tables.wait()
    with jax.named_scope("loads"):
        for load in loads:
            load.wait()
    last.start()

    hops = [(d, h, w) for d in range(1, nc) for h in range(halves) for w in (1, -1)]

    def need(i):
        if i < len(far):
            reach = (1, 0) if i == 0 else max(late[i], plain[i])
            while hops and hops[0][:2] <= reach:
                d, h, w = hops.pop(0)
                run(relay, d, h, near * w)

    n = len(far)

    def step(stage, i):
        if 0 <= i < n:
            run(stage, far[i])

    run(project, own[0], halves, 2)
    need(0)
    for i in range(n + 1):
        step(project, i)
        if i == 0:
            last.wait()
            while hops and hops[0][0] == 1:
                d, h, w = hops.pop(0)
                run(relay, d, h, near * w)
            for job in own[:EARLY]:
                run(reduce, job)
        step(finish, i - 4)
        step(reduce, i - 1)
        step(activate, i - 2)
        if i == n:
            for job in own[EARLY:]:
                run(reduce, job)
        step(mix, i - 3)
        need(i + 1)
    step(activate, n - 1)
    run(activate, own[0])
    step(finish, n - 3)
    step(mix, n - 2)
    for job in own[1:]:
        run(activate, job)
    step(finish, n - 2)
    step(mix, n - 1)
    run(mix, own[0])
    step(finish, n - 1)
    for job in own[1:]:
        run(mix, job)
    for job in own:
        run(finish, job)
    for h in range(halves):
        run(total, h)
    for copy, when in sends:
        if when is None:
            copy.wait_send()
        else:
            pl.when(when)(copy.wait_send)


def solution(mesh):
    n_gx, n_gy = mesh.shape["gx"], mesh.shape["gy"]
    n_hi, n_lo = factor(n_gy)
    per = 2 if n_gx % 2 == 0 else 1
    nc = n_gx // per
    halves = 2

    def body(tokens, gate_blocks, up_blocks, gate_coords, gate_count,
             down_blocks, down_rows, down_coords, down_count):
        rows, width = tokens.shape
        n_model = width // BLOCK
        fb = FF // (BLOCK * n_gx)
        ca = (fb + 1) // 2
        cb = fb - ca
        cap, capd, used = gate_blocks.shape[2], down_blocks.shape[2], down_rows.shape[-1]
        hr = rows // halves
        rp = per * hr // n_gy
        jobs = nc * halves
        cfg = (n_gx, n_gy, n_hi, n_lo, per, nc, halves, rp, hr, n_model, fb, ca,
               cap, used, capd)
        wa, wb = ca * 2 * BLOCK, cb * 2 * BLOCK
        kl, kh, kg = max(n_lo - 1, 1), max(n_hi - 1, 1), max(n_gy - 1, 1)
        kp = max(per - 1, 1)
        tabs = -(-n_model * fb // LANES) + -(-used * n_model // LANES)
        vm, sm, dma = pltpu.VMEM, pltpu.SMEM, pltpu.SemaphoreType.DMA
        hbm = pl.BlockSpec(memory_space=pltpu.HBM)
        return pl.pallas_call(
            functools.partial(kernel, cfg),
            out_shape=pltpu.VMEM((rows, width), BF16),
            in_specs=[hbm] * 9,
            out_specs=pl.BlockSpec(memory_space=pltpu.VMEM),
            scratch_shapes=[
                sm((2, cap), I32),
                sm((1, 1), I32),
                sm((2, capd), I32),
                sm((1, 1), I32),
                sm(down_rows.shape, I32),
                vm((tabs, 1, LANES), I32),
                sm((tabs, 1, LANES), I32),
                vm((cap + 1, BLOCK, BLOCK), BF16),
                vm((cap + 1, BLOCK, BLOCK), BF16),
                vm((capd + 1, BLOCK, BLOCK), BF16),
                vm((nc, halves, per, hr, width), BF16),
                vm((jobs, n_hi, n_lo, rp, wa), BF16),
                vm((jobs, n_hi, n_lo, rp, wb), BF16),
                vm((jobs, kl, n_hi, rp, wa), BF16),
                vm((jobs, kh, n_lo, rp, wb), BF16),
                vm((jobs, kh, rp, wa), BF16),
                vm((jobs, kl, rp, wb), BF16),
                vm((jobs, kh, rp, wa), BF16),
                vm((jobs, kl, rp, wb), BF16),
                vm((jobs, rp, wa), F32),
                vm((jobs, rp, wb), F32),
                vm((fb, rp, BLOCK), BF16),
                vm((jobs, kg, rp, used * BLOCK), BF16),
                vm((jobs, n_gy, rp, used * BLOCK), BF16),
                vm((jobs, per * hr, width), BF16),
                vm((jobs, kp, hr, width), BF16),
                vm((jobs, hr, width), BF16),
                vm((nc, halves, hr, width), BF16),
                vm((halves, hr, width), F32),
                dma((8 + halves,)), dma((2, LOADS)),
                dma((nc, halves, 1 + per)), dma((nc, halves, per)),
                dma((jobs, kl, 2)), dma((jobs, kl, 2)),
                dma((jobs, kh, 2)), dma((jobs, kh, 2)),
                dma((jobs, kh)), dma((jobs, kh)),
                dma((jobs, kl)), dma((jobs, kl)),
                dma((jobs, kg)), dma((jobs, n_gy)),
                dma((jobs,)), dma((nc, halves)),
                dma((jobs, kp)), dma((jobs, kp)),
            ],
            compiler_params=pltpu.CompilerParams(
                collective_id=0, has_side_effects=True, vmem_limit_bytes=60 * 1024 * 1024),
        )(gate_coords[0, 0].T, gate_count, down_coords[0, 0].T, down_count, down_rows,
          tokens, gate_blocks.reshape(cap, BLOCK, BLOCK),
          up_blocks.reshape(cap, BLOCK, BLOCK), down_blocks.reshape(capd, BLOCK, BLOCK))

    return jax.shard_map(
        body,
        mesh=mesh,
        in_specs=(
            P("gx", "gy"),
            P("gy", "gx", None, None, None),
            P("gy", "gx", None, None, None),
            P("gy", "gx", None, None),
            P("gy", "gx"),
            P("gx", "gy", None, None, None),
            P("gx", None, None),
            P("gx", "gy", None, None),
            P("gx", "gy"),
        ),
        out_specs=P("gx", "gy"),
        check_vma=False,
    )
```

```python
import functools

import jax
import jax.numpy as jnp
from jax import lax
from jax.experimental import pallas as pl
from jax.experimental.pallas import tpu as pltpu
from jax.sharding import PartitionSpec as P

BLOCK = 128
LANES = 128
EARLY = 1
FF = 14336
MESH = pl.DeviceIdType.MESH
F32, BF16, I32 = jnp.float32, jnp.bfloat16, jnp.int32


def factor(n):
    low = 1
    while low * low * 4 <= n and n % (low * 2) == 0:
        low *= 2
    return n // low, low


def kernel(cfg, gco_h, gct_h, dco_h, dct_h, kept_h, tok, gblk, ublk, dblk, out,
           gco, gct, dco, dct, kept, tabv, tabs,
           gw, uw, dw, gat, pa, pb,
           r1a, r1b, s2a, s2b, r2a, r2b, acca, accb, hid, a2s, a2r, ps, fp, f2, fr, facc,
           lsem, gs, gr, s1as, s1ar, s1bs, s1br, s2as, s2ar, s2bs, s2br, xs, xr, fs, fq, fps, fpr):
    (n_gx, n_gy, n_hi, n_lo, per, nc, halves, rp, hr, n_model, fb, ca,
     cap, used, capd) = cfg
    gx, gy = lax.axis_index("gx"), lax.axis_index("gy")
    zc, mc = gx // per, gx % per
    hi, lo = gy // n_lo, gy % n_lo
    tall = per * hr
    down_at = -(-n_model * fb // LANES)

    barrier = pltpu.get_barrier_semaphore()

    def greet(dev):
        pl.semaphore_signal(barrier, inc=1, device_id=dev, device_id_type=MESH)

    for d in range(1, n_lo):
        greet((gx, hi * n_lo + (lo + d) % n_lo))
    for d in range(1, n_hi):
        greet((gx, (hi + d) % n_hi * n_lo + lo))
    for d in range(1, per):
        greet((zc * per + (mc + d) % per, gy))

    @pl.when(zc > 0)
    def _():
        greet(((zc - 1) * per + mc, gy))

    @pl.when(zc < nc - 1)
    def _():
        greet(((zc + 1) * per + mc, gy))

    smalls = [
        pltpu.make_async_copy(gco_h, gco, lsem.at[0]),
        pltpu.make_async_copy(gct_h, gct, lsem.at[1]),
        pltpu.make_async_copy(dco_h, dco, lsem.at[2]),
        pltpu.make_async_copy(dct_h, dct, lsem.at[3]),
        pltpu.make_async_copy(kept_h, kept, lsem.at[4]),
    ]
    mine = [
        pltpu.make_async_copy(tok.at[pl.ds(h * hr, hr)], gat.at[zc, h, mc], lsem.at[8 + h])
        for h in range(halves)
    ]
    loads = [
        pltpu.make_async_copy(gblk, gw.at[pl.ds(0, cap)], lsem.at[5]),
        pltpu.make_async_copy(ublk, uw.at[pl.ds(0, cap)], lsem.at[6]),
        pltpu.make_async_copy(dblk, dw.at[pl.ds(0, capd)], lsem.at[7]),
    ]
    for load in smalls + mine + loads[:1]:
        load.start()

    def table(coords, count, slots, inner, spots, first):
        wide = -(-spots // LANES)
        lane = lax.broadcasted_iota(I32, (1, LANES), 1)
        row = [jnp.full((1, LANES), slots, I32) for _ in range(wide)]
        live = count[0, 0]
        for s in range(slots):
            place = coords[0, s] * inner + coords[1, s]
            place = jnp.where(s < live, place, -1)
            for w in range(wide):
                row[w] = jnp.where(lane + w * LANES == place, s, row[w])
        for w in range(wide):
            tabv[first + w] = row[w]

    with jax.named_scope("tables"):
        for load in smalls:
            load.wait()
        table(gco, gct, cap, fb, n_model * fb, 0)
        table(dco, dct, capd, n_model, used * n_model, down_at)
        gw[cap] = jnp.zeros((BLOCK, BLOCK), BF16)
        uw[cap] = jnp.zeros((BLOCK, BLOCK), BF16)
        dw[capd] = jnp.zeros((BLOCK, BLOCK), BF16)
        tables = pltpu.make_async_copy(tabv, tabs, lsem.at[0])
        tables.start()
        loads[1].start()
        for load in mine:
            load.wait()

    with jax.named_scope("barrier"):
        pl.semaphore_wait(
            barrier,
            n_lo + n_hi + per - 3 + jnp.minimum(zc, 1) + jnp.minimum(nc - 1 - zc, 1))

    sends = []

    def send(src, dst, ssem, rsem, dev, when=None):
        copy = pltpu.make_async_remote_copy(
            src_ref=src, dst_ref=dst, send_sem=ssem, recv_sem=rsem,
            device_id=dev, device_id_type=MESH)
        if when is None:
            copy.start()
        else:
            pl.when(when)(copy.start)
        sends.append((copy, when))

    def arrived(ref, sem):
        with jax.named_scope("w"):
            pltpu.make_async_remote_copy(
                src_ref=ref, dst_ref=ref, send_sem=sem, recv_sem=sem,
                device_id=(gx, (gy + 1) % n_gy), device_id_type=MESH).wait_recv()

    near = 1 - 2 * (zc % 2)

    def share(c, h, ways, there=None):
        ref = gat.at[c, h, mc]
        for at, way in enumerate(ways):
            to = zc + way
            fits = (to >= 0) & (to < nc)
            send(ref, ref, gs.at[c, h, at], gr.at[c, h, mc], (to * per + mc, gy),
                 fits if there is None else there & fits)
        for j in range(1, per):
            send(ref, ref, gs.at[c, h, 1 + j], gr.at[c, h, mc],
                 (zc * per + (mc + j) % per, gy), there)

    def relay(d, h, way):
        c = zc + way * d
        there = (c >= 0) & (c < nc)

        @pl.when(there)
        def _():
            arrived(gat.at[c, h, mc], gr.at[c, h, mc])

        share(c, h, (-way,), there)

    own = [(h, zc, h) for h in range(halves)]
    plain = [(k, h) for k in range(1, nc) for h in range(halves)]
    late = plain[:1] + [kh for kh in plain if kh[0] > 1] + plain[1:halves]
    turn = zc % 2 * jnp.minimum(nc - 1 - zc, 1)
    far = []
    for i, (a, b) in enumerate(zip(late, plain)):
        k, h = (u + turn * (v - u) if u != v else u for u, v in zip(a, b))
        far.append((halves + i, zc ^ k, h))

    def spans(many, pieces):
        cut = many // 2
        return [(0, cut), (cut, many)] if pieces == 2 and cut else [(0, many)]

    def project(first_job, count=1, pieces=1, between=None):
        j, chip, h = first_job
        for g in [h + i for i in range(count)]:
            for d in range(1, per):
                c = (mc + d) % per
                arrived(gat.at[chip, g, c], gr.at[chip, g, c])
        parts = ((pa, 0, ca), (pb, ca, fb - ca))
        for piece in range(pieces):
            for part, first, many in parts:
                cuts = spans(many, pieces)
                if piece >= len(cuts):
                    continue
                start, stop = cuts[piece]
                for t in range(start, stop):
                    columns = []
                    for b in (2 * t, 2 * t + 1):
                        ref, c = (gw, b) if b < many else (uw, b - many)
                        at = [r * fb + c + first for r in range(n_model)]
                        columns.append(jnp.concatenate(
                            [ref[tabs[a // LANES, 0, a % LANES]] for a in at], axis=0))
                    x = gat[chip, pl.ds(h, count)].reshape(count * tall, n_model * BLOCK)
                    y = jnp.dot(x, jnp.concatenate(columns, axis=1),
                                preferred_element_type=F32)
                    part[pl.ds(j, count), :, :, :, pl.ds(t * 2 * BLOCK, 2 * BLOCK)] = (
                        y.astype(BF16).reshape(count, n_hi, n_lo, rp, 2 * BLOCK))
                cols = pl.ds(start * 2 * BLOCK, (stop - start) * 2 * BLOCK)
                for g in range(j, j + count):
                    split[g] = pieces
                    if part is pa:
                        for d in range(1, n_lo):
                            l2 = (lo + d) % n_lo
                            send(pa.at[g, :, l2, :, cols], r1a.at[g, d - 1, :, :, cols],
                                 s1as.at[g, d - 1, piece], s1ar.at[g, d - 1, piece],
                                 (gx, hi * n_lo + l2))
                    else:
                        for d in range(1, n_hi):
                            h2 = (hi + d) % n_hi
                            send(pb.at[g, h2, :, :, cols], r1b.at[g, d - 1, :, :, cols],
                                 s1bs.at[g, d - 1, piece], s1br.at[g, d - 1, piece],
                                 (gx, h2 * n_lo + lo))
            if between is not None and piece == 0:
                between()

    split = {}

    def first_arrived(ref, sem, many, pieces):
        for piece, (a, b) in enumerate(spans(many, pieces)):
            cols = pl.ds(a * 2 * BLOCK, (b - a) * 2 * BLOCK)
            arrived(ref.at[:, :, cols], sem.at[piece])

    def reduce(job):
        j = job[0]
        for d in range(1, n_lo):
            first_arrived(r1a.at[j, d - 1], s1ar.at[j, d - 1], ca, split[j])
        for e in list(range(1, n_hi)) + [0]:
            h2 = (hi + e) % n_hi
            s = pa[j, h2, lo].astype(F32)
            for d in range(1, n_lo):
                s = s + r1a[j, d - 1, h2].astype(F32)
            if e == 0:
                acca[j] = s
            else:
                s2a[j, e - 1] = s.astype(BF16)
                send(s2a.at[j, e - 1], r2a.at[j, e - 1], s2as.at[j, e - 1],
                     s2ar.at[j, e - 1], (gx, h2 * n_lo + lo))
        for d in range(1, n_hi):
            first_arrived(r1b.at[j, d - 1], s1br.at[j, d - 1], fb - ca, split[j])
        for e in list(range(1, n_lo)) + [0]:
            l2 = (lo + e) % n_lo
            s = pb[j, hi, l2].astype(F32)
            for d in range(1, n_hi):
                s = s + r1b[j, d - 1, l2].astype(F32)
            if e == 0:
                accb[j] = s
            else:
                s2b[j, e - 1] = s.astype(BF16)
                send(s2b.at[j, e - 1], r2b.at[j, e - 1], s2bs.at[j, e - 1],
                     s2br.at[j, e - 1], (gx, hi * n_lo + l2))

    def activate(job):
        j = job[0]
        for d in range(1, n_hi):
            arrived(r2a.at[j, d - 1], s2ar.at[j, d - 1])
        for d in range(1, n_lo):
            arrived(r2b.at[j, d - 1], s2br.at[j, d - 1])
        for c in range(fb):
            acc, got, peers, at, many = (
                (acca, r2a, n_hi, c, ca) if c < ca else (accb, r2b, n_lo, c - ca, fb - ca))
            both = []
            for b in (at, many + at):
                cols = pl.ds(b * BLOCK, BLOCK)
                v = acc[j, :, cols]
                for d in range(1, peers):
                    v = v + got[j, d - 1, :, cols].astype(F32)
                both.append(v)
            gate, up = both
            hid[c] = (gate / (1.0 + jnp.exp(-gate)) * up).astype(BF16)
        others = [(a, b) for a in range(n_hi) for b in range(n_lo) if a or b]
        others.sort(key=lambda ab: -(ab[0] > 0) - (ab[1] > 0))
        for at, (a, b) in enumerate(others):
            dest = (hi + a) % n_hi * n_lo + (lo + b) % n_lo
            for q in range(used):
                a2s[j, at, :, pl.ds(q * BLOCK, BLOCK)] = hid[kept[0, dest, q]]
            send(a2s.at[j, at], a2r.at[j, gy], xs.at[j, at], xr.at[j, gy], (gx, dest))
        for q in range(used):
            a2r[j, gy, :, pl.ds(q * BLOCK, BLOCK)] = hid[kept[0, gy, q]]

    wide = 2 * BLOCK

    def mix(job):
        j = job[0]
        for d in range(1, n_gy):
            src = (gy + d) % n_gy
            arrived(a2r.at[j, src], xr.at[j, src])

        def col(c, _):
            at = pl.multiple_of(c * wide, wide)
            slots = []
            for r in range(used):
                pair = [r * n_model + c * 2 + i for i in range(2)]
                slots.append([tabs[down_at + p // LANES, 0, p % LANES] for p in pair])
            weight = jnp.concatenate(
                [jnp.concatenate([dw[i] for i in pair], axis=1) for pair in slots], axis=0)
            ps[j, :, pl.ds(at, wide)] = jnp.dot(
                a2r[j].reshape(tall, used * BLOCK), weight,
                preferred_element_type=F32).astype(BF16)
            return 0

        lax.fori_loop(0, n_model * BLOCK // wide, col, 0, unroll=True)
        for d in range(1, per):
            cj = (mc + d) % per
            send(ps.at[j, pl.ds(pl.multiple_of(cj * hr, hr), hr)], fp.at[j, d - 1],
                 fps.at[j, d - 1], fpr.at[j, d - 1], (zc * per + cj, gy))

    def finish(job):
        j, chip, h = job
        s = ps[j, pl.ds(pl.multiple_of(mc * hr, hr), hr)].astype(F32)
        for d in range(1, per):
            arrived(fp.at[j, d - 1], fpr.at[j, d - 1])
            s = s + fp[j, d - 1].astype(F32)
        if j < halves:
            facc[j] = s
        else:
            f2[j] = s.astype(BF16)
            send(f2.at[j], fr.at[zc, h], fs.at[j], fq.at[zc, h], (chip * per + mc, gy))

    def total(h):
        s = facc[h]
        for k in range(1, nc):
            c = zc ^ k
            arrived(fr.at[c, h], fq.at[c, h])
            s = s + fr[c, h].astype(F32)
        out[pl.ds(h * hr, hr)] = s.astype(BF16)

    def run(stage, *args):
        tag = args[0][0] if isinstance(args[0], tuple) else args[0]
        with jax.named_scope(f"{stage.__name__}#j={tag}"):
            stage(*args)

    for h in range(halves):
        share(zc, h, (1, -1))
    tables.wait()
    with jax.named_scope("loads"):
        loads[0].wait()

    hops = [(d, h, w) for d in range(1, nc) for h in range(halves) for w in (1, -1)]

    def need(i):
        if i < len(far):
            reach = (1, 0) if i == 0 else max(late[i], plain[i])
            while hops and hops[0][:2] <= reach:
                d, h, w = hops.pop(0)
                run(relay, d, h, near * w)

    n = len(far)

    def step(stage, i):
        if 0 <= i < n:
            run(stage, far[i])

    def more():
        loads[1].wait()
        loads[2].start()

    run(project, own[0], halves, 2, more)
    need(0)
    for i in range(n + 1):
        step(project, i)
        if i == 0:
            loads[2].wait()
            while hops and hops[0][0] == 1:
                d, h, w = hops.pop(0)
                run(relay, d, h, near * w)
            for job in own[:EARLY]:
                run(reduce, job)
        step(finish, i - 4)
        step(reduce, i - 1)
        step(activate, i - 2)
        if i == n:
            for job in own[EARLY:]:
                run(reduce, job)
        step(mix, i - 3)
        need(i + 1)
    step(activate, n - 1)
    run(activate, own[0])
    step(finish, n - 3)
    step(mix, n - 2)
    for job in own[1:]:
        run(activate, job)
    step(finish, n - 2)
    step(mix, n - 1)
    run(mix, own[0])
    step(finish, n - 1)
    for job in own[1:]:
        run(mix, job)
    for job in own:
        run(finish, job)
    for h in range(halves):
        run(total, h)
    for copy, when in sends:
        if when is None:
            copy.wait_send()
        else:
            pl.when(when)(copy.wait_send)


def solution(mesh):
    n_gx, n_gy = mesh.shape["gx"], mesh.shape["gy"]
    n_hi, n_lo = factor(n_gy)
    per = 2 if n_gx % 2 == 0 else 1
    nc = n_gx // per
    halves = 2

    def body(tokens, gate_blocks, up_blocks, gate_coords, gate_count,
             down_blocks, down_rows, down_coords, down_count):
        rows, width = tokens.shape
        n_model = width // BLOCK
        fb = FF // (BLOCK * n_gx)
        ca = (fb + 1) // 2
        cb = fb - ca
        cap, capd, used = gate_blocks.shape[2], down_blocks.shape[2], down_rows.shape[-1]
        hr = rows // halves
        rp = per * hr // n_gy
        jobs = nc * halves
        cfg = (n_gx, n_gy, n_hi, n_lo, per, nc, halves, rp, hr, n_model, fb, ca,
               cap, used, capd)
        wa, wb = ca * 2 * BLOCK, cb * 2 * BLOCK
        kl, kh, kg = max(n_lo - 1, 1), max(n_hi - 1, 1), max(n_gy - 1, 1)
        kp = max(per - 1, 1)
        tabs = -(-n_model * fb // LANES) + -(-used * n_model // LANES)
        vm, sm, dma = pltpu.VMEM, pltpu.SMEM, pltpu.SemaphoreType.DMA
        hbm = pl.BlockSpec(memory_space=pltpu.HBM)
        return pl.pallas_call(
            functools.partial(kernel, cfg),
            out_shape=pltpu.VMEM((rows, width), BF16),
            in_specs=[hbm] * 9,
            out_specs=pl.BlockSpec(memory_space=pltpu.VMEM),
            scratch_shapes=[
                sm((2, cap), I32),
                sm((1, 1), I32),
                sm((2, capd), I32),
                sm((1, 1), I32),
                sm(down_rows.shape, I32),
                vm((tabs, 1, LANES), I32),
                sm((tabs, 1, LANES), I32),
                vm((cap + 1, BLOCK, BLOCK), BF16),
                vm((cap + 1, BLOCK, BLOCK), BF16),
                vm((capd + 1, BLOCK, BLOCK), BF16),
                vm((nc, halves, per, hr, width), BF16),
                vm((jobs, n_hi, n_lo, rp, wa), BF16),
                vm((jobs, n_hi, n_lo, rp, wb), BF16),
                vm((jobs, kl, n_hi, rp, wa), BF16),
                vm((jobs, kh, n_lo, rp, wb), BF16),
                vm((jobs, kh, rp, wa), BF16),
                vm((jobs, kl, rp, wb), BF16),
                vm((jobs, kh, rp, wa), BF16),
                vm((jobs, kl, rp, wb), BF16),
                vm((jobs, rp, wa), F32),
                vm((jobs, rp, wb), F32),
                vm((fb, rp, BLOCK), BF16),
                vm((jobs, kg, rp, used * BLOCK), BF16),
                vm((jobs, n_gy, rp, used * BLOCK), BF16),
                vm((jobs, per * hr, width), BF16),
                vm((jobs, kp, hr, width), BF16),
                vm((jobs, hr, width), BF16),
                vm((nc, halves, hr, width), BF16),
                vm((halves, hr, width), F32),
                dma((8 + halves,)),
                dma((nc, halves, 1 + per)), dma((nc, halves, per)),
                dma((jobs, kl, 2)), dma((jobs, kl, 2)),
                dma((jobs, kh, 2)), dma((jobs, kh, 2)),
                dma((jobs, kh)), dma((jobs, kh)),
                dma((jobs, kl)), dma((jobs, kl)),
                dma((jobs, kg)), dma((jobs, n_gy)),
                dma((jobs,)), dma((nc, halves)),
                dma((jobs, kp)), dma((jobs, kp)),
            ],
            compiler_params=pltpu.CompilerParams(
                collective_id=0, has_side_effects=True, vmem_limit_bytes=60 * 1024 * 1024),
        )(gate_coords[0, 0].T, gate_count, down_coords[0, 0].T, down_count, down_rows,
          tokens, gate_blocks.reshape(cap, BLOCK, BLOCK),
          up_blocks.reshape(cap, BLOCK, BLOCK), down_blocks.reshape(capd, BLOCK, BLOCK))

    return jax.shard_map(
        body,
        mesh=mesh,
        in_specs=(
            P("gx", "gy"),
            P("gy", "gx", None, None, None),
            P("gy", "gx", None, None, None),
            P("gy", "gx", None, None),
            P("gy", "gx"),
            P("gx", "gy", None, None, None),
            P("gx", None, None),
            P("gx", "gy", None, None),
            P("gx", "gy"),
        ),
        out_specs=P("gx", "gy"),
        check_vma=False,
    )
```

```python
import functools

import jax
import jax.numpy as jnp
from jax import lax
from jax.experimental import pallas as pl
from jax.experimental.pallas import tpu as pltpu
from jax.sharding import PartitionSpec as P

BLOCK = 128
LANES = 128
PIECES = 3
FF = 14336
MESH = pl.DeviceIdType.MESH
F32, BF16, I32 = jnp.float32, jnp.bfloat16, jnp.int32


def factor(n):
    low = 1
    while low * low * 4 <= n and n % (low * 2) == 0:
        low *= 2
    return n // low, low


def kernel(cfg, gco_h, gct_h, dco_h, dct_h, kept_h, tok, gblk, ublk, dblk, out,
           gco, gct, dco, dct, kept, tabv, tabs,
           gw, uw, dw, gat, pa, pb,
           r1a, r1b, s2a, s2b, r2a, r2b, acca, accb, hid, a2s, a2r, ps, fp, f2, fr, facc,
           lsem, gs, gr, s1as, s1ar, s1bs, s1br, s2as, s2ar, s2bs, s2br, xs, xr, fs, fq, fps, fpr):
    (n_gx, n_gy, n_hi, n_lo, per, nc, halves, rp, hr, n_model, fb, ca,
     cap, used, capd) = cfg
    gx, gy = lax.axis_index("gx"), lax.axis_index("gy")
    zc, mc = gx // per, gx % per
    hi, lo = gy // n_lo, gy % n_lo
    tall = per * hr
    down_at = -(-n_model * fb // LANES)

    barrier = pltpu.get_barrier_semaphore()

    def greet(dev):
        pl.semaphore_signal(barrier, inc=1, device_id=dev, device_id_type=MESH)

    for d in range(1, n_lo):
        greet((gx, hi * n_lo + (lo + d) % n_lo))
    for d in range(1, n_hi):
        greet((gx, (hi + d) % n_hi * n_lo + lo))
    for d in range(1, per):
        greet((zc * per + (mc + d) % per, gy))

    @pl.when(zc > 0)
    def _():
        greet(((zc - 1) * per + mc, gy))

    @pl.when(zc < nc - 1)
    def _():
        greet(((zc + 1) * per + mc, gy))

    smalls = [
        pltpu.make_async_copy(gco_h, gco, lsem.at[0]),
        pltpu.make_async_copy(gct_h, gct, lsem.at[1]),
        pltpu.make_async_copy(dco_h, dco, lsem.at[2]),
        pltpu.make_async_copy(dct_h, dct, lsem.at[3]),
        pltpu.make_async_copy(kept_h, kept, lsem.at[4]),
    ]
    mine = [
        pltpu.make_async_copy(tok.at[pl.ds(h * hr, hr)], gat.at[zc, h, mc], lsem.at[8 + h])
        for h in range(halves)
    ]
    loads = [
        pltpu.make_async_copy(gblk, gw.at[pl.ds(0, cap)], lsem.at[5]),
        pltpu.make_async_copy(ublk, uw.at[pl.ds(0, cap)], lsem.at[6]),
        pltpu.make_async_copy(dblk, dw.at[pl.ds(0, capd)], lsem.at[7]),
    ]
    for load in smalls + mine + loads[:1]:
        load.start()

    def table(coords, count, slots, inner, spots, first):
        wide = -(-spots // LANES)
        lane = lax.broadcasted_iota(I32, (1, LANES), 1)
        row = [jnp.full((1, LANES), slots, I32) for _ in range(wide)]
        live = count[0, 0]
        for s in range(slots):
            place = coords[0, s] * inner + coords[1, s]
            place = jnp.where(s < live, place, -1)
            for w in range(wide):
                row[w] = jnp.where(lane + w * LANES == place, s, row[w])
        for w in range(wide):
            tabv[first + w] = row[w]

    with jax.named_scope("tables"):
        for load in smalls:
            load.wait()
        table(gco, gct, cap, fb, n_model * fb, 0)
        table(dco, dct, capd, n_model, used * n_model, down_at)
        gw[cap] = jnp.zeros((BLOCK, BLOCK), BF16)
        uw[cap] = jnp.zeros((BLOCK, BLOCK), BF16)
        dw[capd] = jnp.zeros((BLOCK, BLOCK), BF16)
        tables = pltpu.make_async_copy(tabv, tabs, lsem.at[0])
        tables.start()
        loads[1].start()
        for load in mine:
            load.wait()

    with jax.named_scope("barrier"):
        pl.semaphore_wait(
            barrier,
            n_lo + n_hi + per - 3 + jnp.minimum(zc, 1) + jnp.minimum(nc - 1 - zc, 1))

    sends = []

    def send(src, dst, ssem, rsem, dev, when=None):
        copy = pltpu.make_async_remote_copy(
            src_ref=src, dst_ref=dst, send_sem=ssem, recv_sem=rsem,
            device_id=dev, device_id_type=MESH)
        if when is None:
            copy.start()
        else:
            pl.when(when)(copy.start)
        sends.append((copy, when))

    def arrived(ref, sem):
        with jax.named_scope("w"):
            pltpu.make_async_remote_copy(
                src_ref=ref, dst_ref=ref, send_sem=sem, recv_sem=sem,
                device_id=(gx, (gy + 1) % n_gy), device_id_type=MESH).wait_recv()

    def share(c, h, ways, there=None):
        ref = gat.at[c, h, mc]
        for at, way in enumerate(ways):
            to = zc + way
            fits = (to >= 0) & (to < nc)
            send(ref, ref, gs.at[c, h, at], gr.at[c, h, mc], (to * per + mc, gy),
                 fits if there is None else there & fits)
        for j in range(1, per):
            send(ref, ref, gs.at[c, h, 1 + j], gr.at[c, h, mc],
                 (zc * per + (mc + j) % per, gy), there)

    def relay(d, h, way):
        c = zc + way * d
        there = (c >= 0) & (c < nc)

        @pl.when(there)
        def _():
            arrived(gat.at[c, h, mc], gr.at[c, h, mc])

        share(c, h, (-way,), there)

    own = [(h, zc, h) for h in range(halves)]
    plain = [(k, h) for k in range(1, nc) for h in range(halves)]
    late = plain[:1] + [kh for kh in plain if kh[0] > 1] + plain[1:halves]
    peak = [(k, 0) for k in range(1, nc)] + [
        (k, h) for k in range(nc - 1, 0, -1) for h in range(1, halves)]

    def order(z):
        return peak if z == nc - 1 else plain if z % 2 else late

    top = 1 - jnp.minimum(nc - 1 - zc, 1)
    odd = zc % 2 * (1 - top)
    far = []
    for i, (a, b, c) in enumerate(zip(late, plain, peak)):
        k, h = (u + odd * (v - u) + top * (w - u) for u, v, w in zip(a, b, c))
        far.append((halves + i, zc ^ k, h))

    def spans(many, pieces):
        cut = many // 2
        ends = [0, 1, cut, many] if pieces > 1 and cut > 1 else [0, many]
        return list(zip(ends, ends[1:]))

    def project(first_job, count=1, pieces=1, between=None):
        j, chip, h = first_job
        for g in [h + i for i in range(count)]:
            for d in range(1, per):
                c = (mc + d) % per
                arrived(gat.at[chip, g, c], gr.at[chip, g, c])
        parts = ((pa, 0, ca), (pb, ca, fb - ca))
        for piece in range(pieces):
            for part, first, many in parts:
                cuts = spans(many, pieces)
                if piece >= len(cuts):
                    continue
                start, stop = cuts[piece]
                for t in range(start, stop):
                    columns = []
                    for b in (2 * t, 2 * t + 1):
                        ref, c = (gw, b) if b < many else (uw, b - many)
                        at = [r * fb + c + first for r in range(n_model)]
                        columns.append(jnp.concatenate(
                            [ref[tabs[a // LANES, 0, a % LANES]] for a in at], axis=0))
                    x = gat[chip, pl.ds(h, count)].reshape(count * tall, n_model * BLOCK)
                    y = jnp.dot(x, jnp.concatenate(columns, axis=1),
                                preferred_element_type=F32)
                    part[pl.ds(j, count), :, :, :, pl.ds(t * 2 * BLOCK, 2 * BLOCK)] = (
                        y.astype(BF16).reshape(count, n_hi, n_lo, rp, 2 * BLOCK))
                cols = pl.ds(start * 2 * BLOCK, (stop - start) * 2 * BLOCK)
                for g in range(j, j + count):
                    split[g] = pieces
                    if part is pa:
                        for d in range(1, n_lo):
                            l2 = (lo + d) % n_lo
                            send(pa.at[g, :, l2, :, cols], r1a.at[g, d - 1, :, :, cols],
                                 s1as.at[g, d - 1, piece], s1ar.at[g, d - 1, piece],
                                 (gx, hi * n_lo + l2))
                    else:
                        for d in range(1, n_hi):
                            h2 = (hi + d) % n_hi
                            send(pb.at[g, h2, :, :, cols], r1b.at[g, d - 1, :, :, cols],
                                 s1bs.at[g, d - 1, piece], s1br.at[g, d - 1, piece],
                                 (gx, h2 * n_lo + lo))
            if between is not None and piece == max(pieces - 2, 0):
                between()

    split = {}

    def first_arrived(ref, sem, many, pieces):
        for piece, (a, b) in enumerate(spans(many, pieces)):
            cols = pl.ds(a * 2 * BLOCK, (b - a) * 2 * BLOCK)
            arrived(ref.at[:, :, cols], sem.at[piece])

    def reduce(job):
        j = job[0]
        for d in range(1, n_lo):
            first_arrived(r1a.at[j, d - 1], s1ar.at[j, d - 1], ca, split[j])
        for e in list(range(1, n_hi)) + [0]:
            h2 = (hi + e) % n_hi
            s = pa[j, h2, lo].astype(F32)
            for d in range(1, n_lo):
                s = s + r1a[j, d - 1, h2].astype(F32)
            if e == 0:
                acca[j] = s
            else:
                s2a[j, e - 1] = s.astype(BF16)
                send(s2a.at[j, e - 1], r2a.at[j, e - 1], s2as.at[j, e - 1],
                     s2ar.at[j, e - 1], (gx, h2 * n_lo + lo))
        for d in range(1, n_hi):
            first_arrived(r1b.at[j, d - 1], s1br.at[j, d - 1], fb - ca, split[j])
        for e in list(range(1, n_lo)) + [0]:
            l2 = (lo + e) % n_lo
            s = pb[j, hi, l2].astype(F32)
            for d in range(1, n_hi):
                s = s + r1b[j, d - 1, l2].astype(F32)
            if e == 0:
                accb[j] = s
            else:
                s2b[j, e - 1] = s.astype(BF16)
                send(s2b.at[j, e - 1], r2b.at[j, e - 1], s2bs.at[j, e - 1],
                     s2br.at[j, e - 1], (gx, hi * n_lo + l2))

    def activate(job):
        j = job[0]
        for d in range(1, n_hi):
            arrived(r2a.at[j, d - 1], s2ar.at[j, d - 1])
        for d in range(1, n_lo):
            arrived(r2b.at[j, d - 1], s2br.at[j, d - 1])
        for c in range(fb):
            acc, got, peers, at, many = (
                (acca, r2a, n_hi, c, ca) if c < ca else (accb, r2b, n_lo, c - ca, fb - ca))
            both = []
            for b in (at, many + at):
                cols = pl.ds(b * BLOCK, BLOCK)
                v = acc[j, :, cols]
                for d in range(1, peers):
                    v = v + got[j, d - 1, :, cols].astype(F32)
                both.append(v)
            gate, up = both
            hid[c] = (gate / (1.0 + jnp.exp(-gate)) * up).astype(BF16)
        others = [(a, b) for a in range(n_hi) for b in range(n_lo) if a or b]
        others.sort(key=lambda ab: -(ab[0] > 0) - (ab[1] > 0))
        for at, (a, b) in enumerate(others):
            dest = (hi + a) % n_hi * n_lo + (lo + b) % n_lo
            for q in range(used):
                a2s[j, at, :, pl.ds(q * BLOCK, BLOCK)] = hid[kept[0, dest, q]]
            send(a2s.at[j, at], a2r.at[j, gy], xs.at[j, at], xr.at[j, gy], (gx, dest))
        for q in range(used):
            a2r[j, gy, :, pl.ds(q * BLOCK, BLOCK)] = hid[kept[0, gy, q]]

    wide = 2 * BLOCK

    def mix(job):
        j = job[0]
        for d in range(1, n_gy):
            src = (gy + d) % n_gy
            arrived(a2r.at[j, src], xr.at[j, src])

        def col(c, _):
            at = pl.multiple_of(c * wide, wide)
            slots = []
            for r in range(used):
                pair = [r * n_model + c * 2 + i for i in range(2)]
                slots.append([tabs[down_at + p // LANES, 0, p % LANES] for p in pair])
            weight = jnp.concatenate(
                [jnp.concatenate([dw[i] for i in pair], axis=1) for pair in slots], axis=0)
            ps[j, :, pl.ds(at, wide)] = jnp.dot(
                a2r[j].reshape(tall, used * BLOCK), weight,
                preferred_element_type=F32).astype(BF16)
            return 0

        lax.fori_loop(0, n_model * BLOCK // wide, col, 0, unroll=True)
        for d in range(1, per):
            cj = (mc + d) % per
            send(ps.at[j, pl.ds(pl.multiple_of(cj * hr, hr), hr)], fp.at[j, d - 1],
                 fps.at[j, d - 1], fpr.at[j, d - 1], (zc * per + cj, gy))

    def finish(job):
        j, chip, h = job
        s = ps[j, pl.ds(pl.multiple_of(mc * hr, hr), hr)].astype(F32)
        for d in range(1, per):
            arrived(fp.at[j, d - 1], fpr.at[j, d - 1])
            s = s + fp[j, d - 1].astype(F32)
        if j < halves:
            facc[j] = s
        else:
            f2[j] = s.astype(BF16)
            send(f2.at[j], fr.at[zc, h], fs.at[j], fq.at[zc, h], (chip * per + mc, gy))

    def total(h):
        s = facc[h]
        for k in range(1, nc):
            c = zc ^ k
            arrived(fr.at[c, h], fq.at[c, h])
            s = s + fr[c, h].astype(F32)
        out[pl.ds(h * hr, hr)] = s.astype(BF16)

    def run(stage, *args):
        tag = args[0][0] if isinstance(args[0], tuple) else args[0]
        with jax.named_scope(f"{stage.__name__}#j={tag}"):
            stage(*args)

    for h in range(halves):
        share(zc, h, (1, -1))
    tables.wait()
    with jax.named_scope("loads"):
        loads[0].wait()

    hops = {w: [(d, h) for d in range(1, nc) for h in range(halves)] for w in (-1, 1)}

    def need(i):
        for w in (-1, 1):
            reach = [(1, i)] if i < halves else []
            for z in range(nc if i < len(far) else 0):
                k, h = order(z)[i]
                if ((z ^ k) - z) * w > 0:
                    reach.append((abs((z ^ k) - z), h))
            while hops[w] and reach and hops[w][0] <= max(reach):
                run(relay, *hops[w].pop(0), w)

    n = len(far)

    def step(stage, i):
        if 0 <= i < n:
            run(stage, far[i])

    def more():
        loads[1].wait()
        loads[2].start()

    run(project, own[0], halves, PIECES, more)
    need(0)
    for i in range(n + 1):
        step(project, i)
        if i == 0:
            loads[2].wait()
            for w in (-1, 1):
                run(relay, *hops[w].pop(0), w)
            run(reduce, own[0])
            need(1)
        step(finish, i - 4)
        step(reduce, i - 1)
        step(activate, i - 2)
        if i == n:
            for job in own[1:]:
                run(reduce, job)
        step(mix, i - 3)
        if i:
            need(i + 1)
    step(activate, n - 1)
    run(activate, own[0])
    step(finish, n - 3)
    step(mix, n - 2)
    for job in own[1:]:
        run(activate, job)
    step(finish, n - 2)
    step(mix, n - 1)
    run(mix, own[0])
    step(finish, n - 1)
    for job in own[1:]:
        run(mix, job)
    for job in own:
        run(finish, job)
    for h in range(halves):
        run(total, h)
    for copy, when in sends:
        if when is None:
            copy.wait_send()
        else:
            pl.when(when)(copy.wait_send)


def solution(mesh):
    n_gx, n_gy = mesh.shape["gx"], mesh.shape["gy"]
    n_hi, n_lo = factor(n_gy)
    per = 2 if n_gx % 2 == 0 else 1
    nc = n_gx // per
    halves = 2

    def body(tokens, gate_blocks, up_blocks, gate_coords, gate_count,
             down_blocks, down_rows, down_coords, down_count):
        rows, width = tokens.shape
        n_model = width // BLOCK
        fb = FF // (BLOCK * n_gx)
        ca = (fb + 1) // 2
        cb = fb - ca
        cap, capd, used = gate_blocks.shape[2], down_blocks.shape[2], down_rows.shape[-1]
        hr = rows // halves
        rp = per * hr // n_gy
        jobs = nc * halves
        cfg = (n_gx, n_gy, n_hi, n_lo, per, nc, halves, rp, hr, n_model, fb, ca,
               cap, used, capd)
        wa, wb = ca * 2 * BLOCK, cb * 2 * BLOCK
        kl, kh, kg = max(n_lo - 1, 1), max(n_hi - 1, 1), max(n_gy - 1, 1)
        kp = max(per - 1, 1)
        tabs = -(-n_model * fb // LANES) + -(-used * n_model // LANES)
        vm, sm, dma = pltpu.VMEM, pltpu.SMEM, pltpu.SemaphoreType.DMA
        hbm = pl.BlockSpec(memory_space=pltpu.HBM)
        return pl.pallas_call(
            functools.partial(kernel, cfg),
            out_shape=pltpu.VMEM((rows, width), BF16),
            in_specs=[hbm] * 9,
            out_specs=pl.BlockSpec(memory_space=pltpu.VMEM),
            scratch_shapes=[
                sm((2, cap), I32),
                sm((1, 1), I32),
                sm((2, capd), I32),
                sm((1, 1), I32),
                sm(down_rows.shape, I32),
                vm((tabs, 1, LANES), I32),
                sm((tabs, 1, LANES), I32),
                vm((cap + 1, BLOCK, BLOCK), BF16),
                vm((cap + 1, BLOCK, BLOCK), BF16),
                vm((capd + 1, BLOCK, BLOCK), BF16),
                vm((nc, halves, per, hr, width), BF16),
                vm((jobs, n_hi, n_lo, rp, wa), BF16),
                vm((jobs, n_hi, n_lo, rp, wb), BF16),
                vm((jobs, kl, n_hi, rp, wa), BF16),
                vm((jobs, kh, n_lo, rp, wb), BF16),
                vm((jobs, kh, rp, wa), BF16),
                vm((jobs, kl, rp, wb), BF16),
                vm((jobs, kh, rp, wa), BF16),
                vm((jobs, kl, rp, wb), BF16),
                vm((jobs, rp, wa), F32),
                vm((jobs, rp, wb), F32),
                vm((fb, rp, BLOCK), BF16),
                vm((jobs, kg, rp, used * BLOCK), BF16),
                vm((jobs, n_gy, rp, used * BLOCK), BF16),
                vm((jobs, per * hr, width), BF16),
                vm((jobs, kp, hr, width), BF16),
                vm((jobs, hr, width), BF16),
                vm((nc, halves, hr, width), BF16),
                vm((halves, hr, width), F32),
                dma((8 + halves,)),
                dma((nc, halves, 1 + per)), dma((nc, halves, per)),
                dma((jobs, kl, PIECES)), dma((jobs, kl, PIECES)),
                dma((jobs, kh, PIECES)), dma((jobs, kh, PIECES)),
                dma((jobs, kh)), dma((jobs, kh)),
                dma((jobs, kl)), dma((jobs, kl)),
                dma((jobs, kg)), dma((jobs, n_gy)),
                dma((jobs,)), dma((nc, halves)),
                dma((jobs, kp)), dma((jobs, kp)),
            ],
            compiler_params=pltpu.CompilerParams(
                collective_id=0, has_side_effects=True, vmem_limit_bytes=60 * 1024 * 1024),
        )(gate_coords[0, 0].T, gate_count, down_coords[0, 0].T, down_count, down_rows,
          tokens, gate_blocks.reshape(cap, BLOCK, BLOCK),
          up_blocks.reshape(cap, BLOCK, BLOCK), down_blocks.reshape(capd, BLOCK, BLOCK))

    return jax.shard_map(
        body,
        mesh=mesh,
        in_specs=(
            P("gx", "gy"),
            P("gy", "gx", None, None, None),
            P("gy", "gx", None, None, None),
            P("gy", "gx", None, None),
            P("gy", "gx"),
            P("gx", "gy", None, None, None),
            P("gx", None, None),
            P("gx", "gy", None, None),
            P("gx", "gy"),
        ),
        out_specs=P("gx", "gy"),
        check_vma=False,
    )
```

```python
import functools

import jax
import jax.numpy as jnp
from jax import lax
from jax.experimental import pallas as pl
from jax.experimental.pallas import tpu as pltpu
from jax.sharding import PartitionSpec as P

BLOCK = 128
LANES = 128
PIECES = 3
FF = 14336
MESH = pl.DeviceIdType.MESH
F32, BF16, I32 = jnp.float32, jnp.bfloat16, jnp.int32


def factor(n):
    low = 1
    while low * low * 4 <= n and n % (low * 2) == 0:
        low *= 2
    return n // low, low


def kernel(cfg, gco_h, gct_h, dco_h, dct_h, kept_h, tok, gblk, ublk, dblk, out,
           gco, gct, dco, dct, kept, tabv, tabs,
           gw, uw, dw, gat, pa, pb,
           r1a, r1b, s2a, s2b, r2a, r2b, acca, accb, hid, a2s, a2r, ps, fp, f2, fr, facc,
           lsem, gs, ks, gr, s1as, s1ar, s1bs, s1br, s2as, s2ar, s2bs, s2br, xs, xr, fs, fq, fps, fpr):
    (n_gx, n_gy, n_hi, n_lo, per, nc, halves, rp, hr, n_model, fb, ca,
     cap, used, capd) = cfg
    gx, gy = lax.axis_index("gx"), lax.axis_index("gy")
    zc, mc = gx // per, gx % per
    hi, lo = gy // n_lo, gy % n_lo
    tall = per * hr
    down_at = -(-n_model * fb // LANES)

    barrier = pltpu.get_barrier_semaphore()

    def greet(dev):
        pl.semaphore_signal(barrier, inc=1, device_id=dev, device_id_type=MESH)

    for d in range(1, n_lo):
        greet((gx, hi * n_lo + (lo + d) % n_lo))
    for d in range(1, n_hi):
        greet((gx, (hi + d) % n_hi * n_lo + lo))
    for d in range(1, per):
        greet((zc * per + (mc + d) % per, gy))

    @pl.when(zc > 0)
    def _():
        greet(((zc - 1) * per + mc, gy))

    @pl.when(zc < nc - 1)
    def _():
        greet(((zc + 1) * per + mc, gy))

    smalls = [
        pltpu.make_async_copy(gco_h, gco, lsem.at[0]),
        pltpu.make_async_copy(gct_h, gct, lsem.at[1]),
        pltpu.make_async_copy(dco_h, dco, lsem.at[2]),
        pltpu.make_async_copy(dct_h, dct, lsem.at[3]),
        pltpu.make_async_copy(kept_h, kept, lsem.at[4]),
    ]
    mine = [
        pltpu.make_async_copy(tok.at[pl.ds(h * hr, hr)], gat.at[zc, h, mc], lsem.at[8 + h])
        for h in range(halves)
    ]
    loads = [
        pltpu.make_async_copy(gblk, gw.at[pl.ds(0, cap)], lsem.at[5]),
        pltpu.make_async_copy(ublk, uw.at[pl.ds(0, cap)], lsem.at[6]),
        pltpu.make_async_copy(dblk, dw.at[pl.ds(0, capd)], lsem.at[7]),
    ]
    for load in smalls + mine + loads[:1]:
        load.start()

    def table(coords, count, slots, inner, spots, first):
        wide = -(-spots // LANES)
        lane = lax.broadcasted_iota(I32, (1, LANES), 1)
        row = [jnp.full((1, LANES), slots, I32) for _ in range(wide)]
        live = count[0, 0]
        for s in range(slots):
            place = coords[0, s] * inner + coords[1, s]
            place = jnp.where(s < live, place, -1)
            for w in range(wide):
                row[w] = jnp.where(lane + w * LANES == place, s, row[w])
        for w in range(wide):
            tabv[first + w] = row[w]

    with jax.named_scope("tables"):
        for load in smalls:
            load.wait()
        table(gco, gct, cap, fb, n_model * fb, 0)
        table(dco, dct, capd, n_model, used * n_model, down_at)
        gw[cap] = jnp.zeros((BLOCK, BLOCK), BF16)
        uw[cap] = jnp.zeros((BLOCK, BLOCK), BF16)
        dw[capd] = jnp.zeros((BLOCK, BLOCK), BF16)
        tables = pltpu.make_async_copy(tabv, tabs, lsem.at[0])
        tables.start()
        loads[1].start()
        for load in mine:
            load.wait()

    with jax.named_scope("barrier"):
        pl.semaphore_wait(
            barrier,
            n_lo + n_hi + per - 3 + jnp.minimum(zc, 1) + jnp.minimum(nc - 1 - zc, 1))

    sends = []

    def send(src, dst, ssem, rsem, dev, when=None, listed=False):
        copy = pltpu.make_async_remote_copy(
            src_ref=src, dst_ref=dst, send_sem=ssem, recv_sem=rsem,
            device_id=dev, device_id_type=MESH)
        if when is None:
            copy.start()
        else:
            pl.when(when)(copy.start)
        if listed:
            sends.append((copy, when))

    def left(ref, sem):
        pltpu.make_async_remote_copy(
            src_ref=ref, dst_ref=ref, send_sem=sem, recv_sem=sem,
            device_id=(gx, (gy + 1) % n_gy), device_id_type=MESH).wait_send()

    def arrived(ref, sem):
        with jax.named_scope("w"):
            pltpu.make_async_remote_copy(
                src_ref=ref, dst_ref=ref, send_sem=sem, recv_sem=sem,
                device_id=(gx, (gy + 1) % n_gy), device_id_type=MESH).wait_recv()

    def share(c, h, ways, there=None):
        ref = gat.at[c, h, mc]
        for at, way in enumerate(ways):
            to = zc + way
            fits = (to >= 0) & (to < nc)
            send(ref, ref, gs.at[c, h, at], gr.at[c, h, mc], (to * per + mc, gy),
                 fits if there is None else there & fits, True)
        for j in range(1, per):
            send(ref, ref, ks.at[j - 1], gr.at[c, h, mc],
                 (zc * per + (mc + j) % per, gy), there)

    def relay(d, h, way):
        c = zc + way * d
        there = (c >= 0) & (c < nc)

        @pl.when(there)
        def _():
            arrived(gat.at[c, h, mc], gr.at[c, h, mc])

        share(c, h, (-way,), there)

    own = [(h, zc, h) for h in range(halves)]
    plain = [(k, h) for k in range(1, nc) for h in range(halves)]
    late = plain[:1] + [kh for kh in plain if kh[0] > 1] + plain[1:halves]
    peak = [(k, 0) for k in range(1, nc)] + [
        (k, h) for k in range(nc - 1, 0, -1) for h in range(1, halves)]

    def order(z):
        return peak if z == nc - 1 else plain if z % 2 else late

    top = 1 - jnp.minimum(nc - 1 - zc, 1)
    odd = zc % 2 * (1 - top)
    far = []
    for i, (a, b, c) in enumerate(zip(late, plain, peak)):
        k, h = (u + odd * (v - u) + top * (w - u) for u, v, w in zip(a, b, c))
        far.append((halves + i, zc ^ k, h))

    def spans(many, pieces):
        cut = many // 2
        ends = [0, 1, cut, many] if pieces > 1 and cut > 1 else [0, many]
        return list(zip(ends, ends[1:]))

    def project(first_job, count=1, pieces=1, between=None):
        j, chip, h = first_job
        for g in [h + i for i in range(count)]:
            for d in range(1, per):
                c = (mc + d) % per
                arrived(gat.at[chip, g, c], gr.at[chip, g, c])
        parts = ((pa, 0, ca), (pb, ca, fb - ca))
        for piece in range(pieces):
            for part, first, many in parts:
                cuts = spans(many, pieces)
                if piece >= len(cuts):
                    continue
                start, stop = cuts[piece]
                for t in range(start, stop):
                    columns = []
                    for b in (2 * t, 2 * t + 1):
                        ref, c = (gw, b) if b < many else (uw, b - many)
                        at = [r * fb + c + first for r in range(n_model)]
                        columns.append(jnp.concatenate(
                            [ref[tabs[a // LANES, 0, a % LANES]] for a in at], axis=0))
                    x = gat[chip, pl.ds(h, count)].reshape(count * tall, n_model * BLOCK)
                    y = jnp.dot(x, jnp.concatenate(columns, axis=1),
                                preferred_element_type=F32)
                    part[pl.ds(j, count), :, :, :, pl.ds(t * 2 * BLOCK, 2 * BLOCK)] = (
                        y.astype(BF16).reshape(count, n_hi, n_lo, rp, 2 * BLOCK))
                cols = pl.ds(start * 2 * BLOCK, (stop - start) * 2 * BLOCK)
                for g in range(j, j + count):
                    if part is pa:
                        for d in range(1, n_lo):
                            l2 = (lo + d) % n_lo
                            send(pa.at[g, :, l2, :, cols], r1a.at[g, d - 1, :, :, cols],
                                 s1as.at[0], s1ar.at[g],
                                 (gx, hi * n_lo + l2))
                    else:
                        for d in range(1, n_hi):
                            h2 = (hi + d) % n_hi
                            send(pb.at[g, h2, :, :, cols], r1b.at[g, d - 1, :, :, cols],
                                 s1bs.at[0], s1br.at[g],
                                 (gx, h2 * n_lo + lo))
            if between is not None and piece == max(pieces - 2, 0):
                between()

    def reduce(job):
        j = job[0]
        if n_lo > 1:
            arrived(r1a.at[j], s1ar.at[j])
        for e in list(range(1, n_hi)) + [0]:
            h2 = (hi + e) % n_hi
            s = pa[j, h2, lo].astype(F32)
            for d in range(1, n_lo):
                s = s + r1a[j, d - 1, h2].astype(F32)
            if e == 0:
                acca[j] = s
            else:
                s2a[j, e - 1] = s.astype(BF16)
                send(s2a.at[j, e - 1], r2a.at[j, e - 1], s2as.at[0], s2ar.at[j],
                     (gx, h2 * n_lo + lo))
        if n_hi > 1:
            arrived(r1b.at[j], s1br.at[j])
        for e in list(range(1, n_lo)) + [0]:
            l2 = (lo + e) % n_lo
            s = pb[j, hi, l2].astype(F32)
            for d in range(1, n_hi):
                s = s + r1b[j, d - 1, l2].astype(F32)
            if e == 0:
                accb[j] = s
            else:
                s2b[j, e - 1] = s.astype(BF16)
                send(s2b.at[j, e - 1], r2b.at[j, e - 1], s2bs.at[0], s2br.at[j],
                     (gx, hi * n_lo + l2))

    def activate(job):
        j = job[0]
        if n_hi > 1:
            arrived(r2a.at[j], s2ar.at[j])
        if n_lo > 1:
            arrived(r2b.at[j], s2br.at[j])
        for c in range(fb):
            acc, got, peers, at, many = (
                (acca, r2a, n_hi, c, ca) if c < ca else (accb, r2b, n_lo, c - ca, fb - ca))
            both = []
            for b in (at, many + at):
                cols = pl.ds(b * BLOCK, BLOCK)
                v = acc[j, :, cols]
                for d in range(1, peers):
                    v = v + got[j, d - 1, :, cols].astype(F32)
                both.append(v)
            gate, up = both
            hid[c] = (gate / (1.0 + jnp.exp(-gate)) * up).astype(BF16)
        others = [(a, b) for a in range(n_hi) for b in range(n_lo) if a or b]
        others.sort(key=lambda ab: -(ab[0] > 0) - (ab[1] > 0))
        for at, (a, b) in enumerate(others):
            dest = (hi + a) % n_hi * n_lo + (lo + b) % n_lo
            for q in range(used):
                a2s[j, at, :, pl.ds(q * BLOCK, BLOCK)] = hid[kept[0, dest, q]]
            send(a2s.at[j, at], a2r.at[j, gy], xs.at[0], xr.at[j], (gx, dest))
        for q in range(used):
            a2r[j, gy, :, pl.ds(q * BLOCK, BLOCK)] = hid[kept[0, gy, q]]

    wide = 2 * BLOCK

    def mix(job):
        j = job[0]
        if n_gy > 1:
            arrived(a2s.at[j], xr.at[j])

        def col(c, _):
            at = pl.multiple_of(c * wide, wide)
            slots = []
            for r in range(used):
                pair = [r * n_model + c * 2 + i for i in range(2)]
                slots.append([tabs[down_at + p // LANES, 0, p % LANES] for p in pair])
            weight = jnp.concatenate(
                [jnp.concatenate([dw[i] for i in pair], axis=1) for pair in slots], axis=0)
            ps[j, :, pl.ds(at, wide)] = jnp.dot(
                a2r[j].reshape(tall, used * BLOCK), weight,
                preferred_element_type=F32).astype(BF16)
            return 0

        lax.fori_loop(0, n_model * BLOCK // wide, col, 0, unroll=True)
        for d in range(1, per):
            cj = (mc + d) % per
            send(ps.at[j, pl.ds(pl.multiple_of(cj * hr, hr), hr)], fp.at[j, d - 1],
                 fps.at[0], fpr.at[j], (zc * per + cj, gy))

    def finish(job):
        j, chip, h = job
        s = ps[j, pl.ds(pl.multiple_of(mc * hr, hr), hr)].astype(F32)
        if per > 1:
            arrived(fp.at[j], fpr.at[j])
        for d in range(1, per):
            s = s + fp[j, d - 1].astype(F32)
        if j < halves:
            facc[j] = s
        else:
            f2[j] = s.astype(BF16)
            send(f2.at[j], fr.at[zc, h], fs.at[0], fq.at[zc, h], (chip * per + mc, gy))

    def total(h):
        s = facc[h]
        for k in range(1, nc):
            c = zc ^ k
            arrived(fr.at[c, h], fq.at[c, h])
            s = s + fr[c, h].astype(F32)
        out[pl.ds(h * hr, hr)] = s.astype(BF16)

    def run(stage, *args):
        tag = args[0][0] if isinstance(args[0], tuple) else args[0]
        with jax.named_scope(f"{stage.__name__}#j={tag}"):
            stage(*args)

    for h in range(halves):
        share(zc, h, (1, -1))
    tables.wait()
    with jax.named_scope("loads"):
        loads[0].wait()

    hops = {w: [(d, h) for d in range(1, nc) for h in range(halves)] for w in (-1, 1)}

    def need(i):
        for w in (-1, 1):
            reach = [(1, i)] if i < halves else []
            for z in range(nc if i < len(far) else 0):
                k, h = order(z)[i]
                if ((z ^ k) - z) * w > 0:
                    reach.append((abs((z ^ k) - z), h))
            while hops[w] and reach and hops[w][0] <= max(reach):
                run(relay, *hops[w].pop(0), w)

    n = len(far)

    def step(stage, i):
        if 0 <= i < n:
            run(stage, far[i])

    def more():
        loads[1].wait()
        loads[2].start()

    run(project, own[0], halves, PIECES, more)
    need(0)
    for i in range(n + 1):
        step(project, i)
        if i == 0:
            loads[2].wait()
            for w in (-1, 1):
                run(relay, *hops[w].pop(0), w)
            run(reduce, own[0])
            need(1)
        step(finish, i - 4)
        step(reduce, i - 1)
        step(activate, i - 2)
        if i == n:
            for job in own[1:]:
                run(reduce, job)
        step(mix, i - 3)
        if i:
            need(i + 1)
    step(activate, n - 1)
    run(activate, own[0])
    step(finish, n - 3)
    step(mix, n - 2)
    for job in own[1:]:
        run(activate, job)
    step(finish, n - 2)
    step(mix, n - 1)
    run(mix, own[0])
    step(finish, n - 1)
    for job in own[1:]:
        run(mix, job)
    for job in own:
        run(finish, job)
    for h in range(halves):
        run(total, h)
    for copy, when in sends:
        if when is None:
            copy.wait_send()
        else:
            pl.when(when)(copy.wait_send)
    for many, ref, sem in (
            (per, gat.at[:, :, 0], None), (n_lo, r1a, s1as), (n_hi, r1b, s1bs),
            (n_hi, s2a, s2as), (n_lo, s2b, s2bs), (n_gy, a2s, xs), (per, fp, fps),
            (nc, f2.at[pl.ds(halves, n)], fs)):
        if many > 1 and sem is not None:
            left(ref, sem.at[0])
        elif many > 1:
            for j in range(1, per):
                left(ref, ks.at[j - 1])


def solution(mesh):
    n_gx, n_gy = mesh.shape["gx"], mesh.shape["gy"]
    n_hi, n_lo = factor(n_gy)
    per = 2 if n_gx % 2 == 0 else 1
    nc = n_gx // per
    halves = 2

    def body(tokens, gate_blocks, up_blocks, gate_coords, gate_count,
             down_blocks, down_rows, down_coords, down_count):
        rows, width = tokens.shape
        n_model = width // BLOCK
        fb = FF // (BLOCK * n_gx)
        ca = (fb + 1) // 2
        cb = fb - ca
        cap, capd, used = gate_blocks.shape[2], down_blocks.shape[2], down_rows.shape[-1]
        hr = rows // halves
        rp = per * hr // n_gy
        jobs = nc * halves
        cfg = (n_gx, n_gy, n_hi, n_lo, per, nc, halves, rp, hr, n_model, fb, ca,
               cap, used, capd)
        wa, wb = ca * 2 * BLOCK, cb * 2 * BLOCK
        kl, kh, kg = max(n_lo - 1, 1), max(n_hi - 1, 1), max(n_gy - 1, 1)
        kp = max(per - 1, 1)
        tabs = -(-n_model * fb // LANES) + -(-used * n_model // LANES)
        vm, sm, dma = pltpu.VMEM, pltpu.SMEM, pltpu.SemaphoreType.DMA
        hbm = pl.BlockSpec(memory_space=pltpu.HBM)
        return pl.pallas_call(
            functools.partial(kernel, cfg),
            out_shape=pltpu.VMEM((rows, width), BF16),
            in_specs=[hbm] * 9,
            out_specs=pl.BlockSpec(memory_space=pltpu.VMEM),
            scratch_shapes=[
                sm((2, cap), I32),
                sm((1, 1), I32),
                sm((2, capd), I32),
                sm((1, 1), I32),
                sm(down_rows.shape, I32),
                vm((tabs, 1, LANES), I32),
                sm((tabs, 1, LANES), I32),
                vm((cap + 1, BLOCK, BLOCK), BF16),
                vm((cap + 1, BLOCK, BLOCK), BF16),
                vm((capd + 1, BLOCK, BLOCK), BF16),
                vm((nc, halves, per, hr, width), BF16),
                vm((jobs, n_hi, n_lo, rp, wa), BF16),
                vm((jobs, n_hi, n_lo, rp, wb), BF16),
                vm((jobs, kl, n_hi, rp, wa), BF16),
                vm((jobs, kh, n_lo, rp, wb), BF16),
                vm((jobs, kh, rp, wa), BF16),
                vm((jobs, kl, rp, wb), BF16),
                vm((jobs, kh, rp, wa), BF16),
                vm((jobs, kl, rp, wb), BF16),
                vm((jobs, rp, wa), F32),
                vm((jobs, rp, wb), F32),
                vm((fb, rp, BLOCK), BF16),
                vm((jobs, kg, rp, used * BLOCK), BF16),
                vm((jobs, n_gy, rp, used * BLOCK), BF16),
                vm((jobs, per * hr, width), BF16),
                vm((jobs, kp, hr, width), BF16),
                vm((jobs, hr, width), BF16),
                vm((nc, halves, hr, width), BF16),
                vm((halves, hr, width), F32),
                dma((8 + halves,)),
                dma((nc, halves, 2)), dma((kp,)), dma((nc, halves, per)),
                dma((1,)), dma((jobs,)),
                dma((1,)), dma((jobs,)),
                dma((1,)), dma((jobs,)),
                dma((1,)), dma((jobs,)),
                dma((1,)), dma((jobs,)),
                dma((1,)), dma((nc, halves)),
                dma((1,)), dma((jobs,)),
            ],
            compiler_params=pltpu.CompilerParams(
                collective_id=0, has_side_effects=True, vmem_limit_bytes=60 * 1024 * 1024),
        )(gate_coords[0, 0].T, gate_count, down_coords[0, 0].T, down_count, down_rows,
          tokens, gate_blocks.reshape(cap, BLOCK, BLOCK),
          up_blocks.reshape(cap, BLOCK, BLOCK), down_blocks.reshape(capd, BLOCK, BLOCK))

    return jax.shard_map(
        body,
        mesh=mesh,
        in_specs=(
            P("gx", "gy"),
            P("gy", "gx", None, None, None),
            P("gy", "gx", None, None, None),
            P("gy", "gx", None, None),
            P("gy", "gx"),
            P("gx", "gy", None, None, None),
            P("gx", None, None),
            P("gx", "gy", None, None),
            P("gx", "gy"),
        ),
        out_specs=P("gx", "gy"),
        check_vma=False,
    )
```

```python
import functools

import jax
import jax.numpy as jnp
from jax import lax
from jax.experimental import pallas as pl
from jax.experimental.pallas import tpu as pltpu
from jax.sharding import PartitionSpec as P

BLOCK = 128
LANES = 128
PIECES = 3
FF = 14336
MESH = pl.DeviceIdType.MESH
F32, BF16, I32 = jnp.float32, jnp.bfloat16, jnp.int32


def factor(n):
    low = 1
    while low * low * 4 <= n and n % (low * 2) == 0:
        low *= 2
    return n // low, low


def kernel(cfg, gco_h, gct_h, dco_h, dct_h, kept_h, tok, gblk, ublk, dblk, out,
           gco, gct, dco, dct, kept, tabv, tabs,
           gw, uw, dw, gat, pa, pb,
           r1a, r1b, s2a, s2b, r2a, r2b, acca, accb, hid, a2s, a2r, ps, fp, f2, fr, facc,
           lsem, gs, ks, gr, s1as, s1ar, s1bs, s1br, s2as, s2ar, s2bs, s2br, xs, xr, fs, fq, fps, fpr):
    (n_gx, n_gy, n_hi, n_lo, per, nc, halves, rp, hr, n_model, fb, ca,
     cap, used, capd) = cfg
    gx, gy = lax.axis_index("gx"), lax.axis_index("gy")
    zc, mc = gx // per, gx % per
    hi, lo = gy // n_lo, gy % n_lo
    tall = per * hr
    down_at = -(-n_model * fb // LANES)

    barrier = pltpu.get_barrier_semaphore()

    def greet(dev):
        pl.semaphore_signal(barrier, inc=1, device_id=dev, device_id_type=MESH)

    for d in range(1, n_lo):
        greet((gx, hi * n_lo + (lo + d) % n_lo))
    for d in range(1, n_hi):
        greet((gx, (hi + d) % n_hi * n_lo + lo))
    for d in range(1, per):
        greet((zc * per + (mc + d) % per, gy))

    @pl.when(zc > 0)
    def _():
        greet(((zc - 1) * per + mc, gy))

    @pl.when(zc < nc - 1)
    def _():
        greet(((zc + 1) * per + mc, gy))

    smalls = [
        pltpu.make_async_copy(gco_h, gco, lsem.at[0]),
        pltpu.make_async_copy(gct_h, gct, lsem.at[1]),
        pltpu.make_async_copy(dco_h, dco, lsem.at[2]),
        pltpu.make_async_copy(dct_h, dct, lsem.at[3]),
        pltpu.make_async_copy(kept_h, kept, lsem.at[4]),
    ]
    mine = [
        pltpu.make_async_copy(tok.at[pl.ds(h * hr, hr)], gat.at[zc, h, mc], lsem.at[8 + h])
        for h in range(halves)
    ]
    loads = [
        pltpu.make_async_copy(gblk, gw.at[pl.ds(0, cap)], lsem.at[5]),
        pltpu.make_async_copy(ublk, uw.at[pl.ds(0, cap)], lsem.at[6]),
        pltpu.make_async_copy(dblk, dw.at[pl.ds(0, capd)], lsem.at[7]),
    ]
    for load in smalls + mine + loads[:1]:
        load.start()

    def table(coords, count, slots, inner, spots, first):
        wide = -(-spots // LANES)
        lane = lax.broadcasted_iota(I32, (1, LANES), 1)
        row = [jnp.full((1, LANES), slots, I32) for _ in range(wide)]
        live = count[0, 0]
        for s in range(slots):
            place = coords[0, s] * inner + coords[1, s]
            place = jnp.where(s < live, place, -1)
            for w in range(wide):
                row[w] = jnp.where(lane + w * LANES == place, s, row[w])
        for w in range(wide):
            tabv[first + w] = row[w]

    with jax.named_scope("tables"):
        for load in smalls:
            load.wait()
        table(gco, gct, cap, fb, n_model * fb, 0)
        table(dco, dct, capd, n_model, used * n_model, down_at)
        gw[cap] = jnp.zeros((BLOCK, BLOCK), BF16)
        uw[cap] = jnp.zeros((BLOCK, BLOCK), BF16)
        dw[capd] = jnp.zeros((BLOCK, BLOCK), BF16)
        tables = pltpu.make_async_copy(tabv, tabs, lsem.at[0])
        tables.start()
        loads[1].start()
        for load in mine:
            load.wait()

    with jax.named_scope("barrier"):
        pl.semaphore_wait(
            barrier,
            n_lo + n_hi + per - 3 + jnp.minimum(zc, 1) + jnp.minimum(nc - 1 - zc, 1))

    sends = []

    def send(src, dst, ssem, rsem, dev, when=None, listed=False):
        copy = pltpu.make_async_remote_copy(
            src_ref=src, dst_ref=dst, send_sem=ssem, recv_sem=rsem,
            device_id=dev, device_id_type=MESH)
        if when is None:
            copy.start()
        else:
            pl.when(when)(copy.start)
        if listed:
            sends.append((copy, when))

    def left(ref, sem):
        pltpu.make_async_remote_copy(
            src_ref=ref, dst_ref=ref, send_sem=sem, recv_sem=sem,
            device_id=(gx, (gy + 1) % n_gy), device_id_type=MESH).wait_send()

    def arrived(ref, sem):
        with jax.named_scope("w"):
            pltpu.make_async_remote_copy(
                src_ref=ref, dst_ref=ref, send_sem=sem, recv_sem=sem,
                device_id=(gx, (gy + 1) % n_gy), device_id_type=MESH).wait_recv()

    def share(c, h, ways, there=None):
        ref = gat.at[c, h, mc]
        for at, way in enumerate(ways):
            to = zc + way
            fits = (to >= 0) & (to < nc)
            send(ref, ref, gs.at[c, h, at], gr.at[c, h, mc], (to * per + mc, gy),
                 fits if there is None else there & fits, True)
        for j in range(1, per):
            send(ref, ref, ks.at[j - 1], gr.at[c, h, mc],
                 (zc * per + (mc + j) % per, gy), there)

    def relay(d, h, way):
        c = zc + way * d
        there = (c >= 0) & (c < nc)

        @pl.when(there)
        def _():
            arrived(gat.at[c, h, mc], gr.at[c, h, mc])

        share(c, h, (-way,), there)

    own = [(h, zc, h) for h in range(halves)]
    plain = [(k, h) for k in range(1, nc) for h in range(halves)]
    late = plain[:1] + [kh for kh in plain if kh[0] > 1] + plain[1:halves]
    peak = [(k, 0) for k in range(1, nc)] + [
        (k, h) for k in range(nc - 1, 0, -1) for h in range(1, halves)]

    def order(z):
        return peak if z == nc - 1 else plain if z % 2 else late

    top = 1 - jnp.minimum(nc - 1 - zc, 1)
    odd = zc % 2 * (1 - top)
    far = []
    for i, (a, b, c) in enumerate(zip(late, plain, peak)):
        k, h = (u + odd * (v - u) + top * (w - u) for u, v, w in zip(a, b, c))
        far.append((halves + i, zc ^ k, h))

    def spans(many, pieces):
        cut = many // 2
        ends = [0, 1, cut, many] if pieces > 1 and cut > 1 else [0, many]
        return list(zip(ends, ends[1:]))

    def project(first_job, count=1, pieces=1, between=None):
        j, chip, h = first_job
        for g in [h + i for i in range(count)]:
            for d in range(1, per):
                c = (mc + d) % per
                arrived(gat.at[chip, g, c], gr.at[chip, g, c])
        parts = ((pa, 0, ca), (pb, ca, fb - ca))
        for piece in range(pieces):
            for part, first, many in parts:
                cuts = spans(many, pieces)
                if piece >= len(cuts):
                    continue
                start, stop = cuts[piece]
                for t in range(start, stop):
                    columns = []
                    for b in (2 * t, 2 * t + 1):
                        ref, c = (gw, b) if b < many else (uw, b - many)
                        at = [r * fb + c + first for r in range(n_model)]
                        columns.append(jnp.concatenate(
                            [ref[tabs[a // LANES, 0, a % LANES]] for a in at], axis=0))
                    x = gat[chip, pl.ds(h, count)].reshape(count * tall, n_model * BLOCK)
                    y = jnp.dot(x, jnp.concatenate(columns, axis=1),
                                preferred_element_type=F32)
                    part[pl.ds(j, count), :, :, :, pl.ds(t * 2 * BLOCK, 2 * BLOCK)] = (
                        y.astype(BF16).reshape(count, n_hi, n_lo, rp, 2 * BLOCK))
                cols = pl.ds(start * 2 * BLOCK, (stop - start) * 2 * BLOCK)
                for g in range(j, j + count):
                    if part is pa:
                        for d in range(1, n_lo):
                            l2 = (lo + d) % n_lo
                            send(pa.at[g, :, l2, :, cols], r1a.at[g, d - 1, :, :, cols],
                                 s1as.at[0], s1ar.at[g],
                                 (gx, hi * n_lo + l2))
                    else:
                        for d in range(1, n_hi):
                            h2 = (hi + d) % n_hi
                            send(pb.at[g, h2, :, :, cols], r1b.at[g, d - 1, :, :, cols],
                                 s1bs.at[0], s1br.at[g],
                                 (gx, h2 * n_lo + lo))
            if between is not None and piece == max(pieces - 2, 0):
                between()

    def reduce(job):
        j = job[0]
        if n_lo > 1:
            arrived(r1a.at[j], s1ar.at[j])
        for e in list(range(1, n_hi)) + [0]:
            h2 = (hi + e) % n_hi
            s = pa[j, h2, lo].astype(F32)
            for d in range(1, n_lo):
                s = s + r1a[j, d - 1, h2].astype(F32)
            if e == 0:
                acca[j] = s
            else:
                s2a[j, e - 1] = s.astype(BF16)
                send(s2a.at[j, e - 1], r2a.at[j, e - 1], s2as.at[0], s2ar.at[j],
                     (gx, h2 * n_lo + lo))
        if n_hi > 1:
            arrived(r1b.at[j], s1br.at[j])
        for e in list(range(1, n_lo)) + [0]:
            l2 = (lo + e) % n_lo
            s = pb[j, hi, l2].astype(F32)
            for d in range(1, n_hi):
                s = s + r1b[j, d - 1, l2].astype(F32)
            if e == 0:
                accb[j] = s
            else:
                s2b[j, e - 1] = s.astype(BF16)
                send(s2b.at[j, e - 1], r2b.at[j, e - 1], s2bs.at[0], s2br.at[j],
                     (gx, hi * n_lo + l2))

    def activate(job):
        j = job[0]
        if n_hi > 1:
            arrived(r2a.at[j], s2ar.at[j])
        if n_lo > 1:
            arrived(r2b.at[j], s2br.at[j])
        for c in range(fb):
            acc, got, peers, at, many = (
                (acca, r2a, n_hi, c, ca) if c < ca else (accb, r2b, n_lo, c - ca, fb - ca))
            both = []
            for b in (at, many + at):
                cols = pl.ds(b * BLOCK, BLOCK)
                v = acc[j, :, cols]
                for d in range(1, peers):
                    v = v + got[j, d - 1, :, cols].astype(F32)
                both.append(v)
            gate, up = both
            hid[c] = (gate / (1.0 + jnp.exp(-gate)) * up).astype(BF16)
        others = [(a, b) for a in range(n_hi) for b in range(n_lo) if a or b]
        others.sort(key=lambda ab: -(ab[0] > 0) - (ab[1] > 0))
        for at, (a, b) in enumerate(others):
            dest = (hi + a) % n_hi * n_lo + (lo + b) % n_lo
            for q in range(used):
                a2s[j, at, :, pl.ds(q * BLOCK, BLOCK)] = hid[kept[0, dest, q]]
            send(a2s.at[j, at], a2r.at[j, gy], xs.at[0], xr.at[j], (gx, dest))
        for q in range(used):
            a2r[j, gy, :, pl.ds(q * BLOCK, BLOCK)] = hid[kept[0, gy, q]]

    wide = 2 * BLOCK

    def mix(job):
        j = job[0]
        if n_gy > 1:
            arrived(a2s.at[j], xr.at[j])

        def col(c, _):
            at = pl.multiple_of(c * wide, wide)
            slots = []
            for r in range(used):
                pair = [r * n_model + c * 2 + i for i in range(2)]
                slots.append([tabs[down_at + p // LANES, 0, p % LANES] for p in pair])
            weight = jnp.concatenate(
                [jnp.concatenate([dw[i] for i in pair], axis=1) for pair in slots], axis=0)
            ps[j, :, pl.ds(at, wide)] = jnp.dot(
                a2r[j].reshape(tall, used * BLOCK), weight,
                preferred_element_type=F32).astype(BF16)
            return 0

        lax.fori_loop(0, n_model * BLOCK // wide, col, 0, unroll=True)
        for d in range(1, per):
            cj = (mc + d) % per
            send(ps.at[j, pl.ds(pl.multiple_of(cj * hr, hr), hr)], fp.at[j, d - 1],
                 fps.at[0], fpr.at[j], (zc * per + cj, gy))

    def finish(job):
        j, chip, h = job
        s = ps[j, pl.ds(pl.multiple_of(mc * hr, hr), hr)].astype(F32)
        if per > 1:
            arrived(fp.at[j], fpr.at[j])
        for d in range(1, per):
            s = s + fp[j, d - 1].astype(F32)
        if j < halves:
            facc[j] = s
        else:
            f2[j] = s.astype(BF16)
            send(f2.at[j], fr.at[zc, h], fs.at[0], fq.at[h], (chip * per + mc, gy))

    def total(h):
        s = facc[h]
        if nc > 1:
            arrived(fr.at[pl.ds(0, nc - 1), h], fq.at[h])
        for k in range(1, nc):
            c = zc ^ k
            s = s + fr[c, h].astype(F32)
        out[pl.ds(h * hr, hr)] = s.astype(BF16)

    def run(stage, *args):
        tag = args[0][0] if isinstance(args[0], tuple) else args[0]
        with jax.named_scope(f"{stage.__name__}#j={tag}"):
            stage(*args)

    for h in range(halves):
        share(zc, h, (1, -1))
    tables.wait()
    with jax.named_scope("loads"):
        loads[0].wait()

    hops = {w: [(d, h) for d in range(1, nc) for h in range(halves)] for w in (-1, 1)}

    def need(i):
        for w in (-1, 1):
            reach = [(1, i)] if i < halves else []
            for z in range(nc if i < len(far) else 0):
                k, h = order(z)[i]
                if ((z ^ k) - z) * w > 0:
                    reach.append((abs((z ^ k) - z), h))
            while hops[w] and reach and hops[w][0] <= max(reach):
                run(relay, *hops[w].pop(0), w)

    n = len(far)

    def step(stage, i, *args):
        if 0 <= i < n:
            run(stage, far[i], *args)

    def more():
        loads[1].wait()
        loads[2].start()

    run(project, own[0], halves, PIECES, more)
    need(0)
    for i in range(n + 1):
        step(project, i, 1, PIECES)
        if i == 0:
            loads[2].wait()
            for w in (-1, 1):
                run(relay, *hops[w].pop(0), w)
            run(reduce, own[0])
            need(1)
        step(finish, i - 4)
        step(reduce, i - 1)
        step(activate, i - 2)
        if i == n:
            for job in own[1:]:
                run(reduce, job)
        step(mix, i - 3)
        if i:
            need(i + 1)
    step(activate, n - 1)
    run(activate, own[0])
    step(finish, n - 3)
    step(mix, n - 2)
    for job in own[1:]:
        run(activate, job)
    step(finish, n - 2)
    step(mix, n - 1)
    run(mix, own[0])
    step(finish, n - 1)
    for job in own[1:]:
        run(mix, job)
    for job in own:
        run(finish, job)
    for h in range(halves):
        run(total, h)
    for copy, when in sends:
        if when is None:
            copy.wait_send()
        else:
            pl.when(when)(copy.wait_send)
    for many, ref, sem in (
            (per, gat.at[:, :, 0], None), (n_lo, r1a, s1as), (n_hi, r1b, s1bs),
            (n_hi, s2a, s2as), (n_lo, s2b, s2bs), (n_gy, a2s, xs), (per, fp, fps),
            (nc, f2.at[pl.ds(halves, n)], fs)):
        if many > 1 and sem is not None:
            left(ref, sem.at[0])
        elif many > 1:
            for j in range(1, per):
                left(ref, ks.at[j - 1])


def solution(mesh):
    n_gx, n_gy = mesh.shape["gx"], mesh.shape["gy"]
    n_hi, n_lo = factor(n_gy)
    per = 2 if n_gx % 2 == 0 else 1
    nc = n_gx // per
    halves = 2

    def body(tokens, gate_blocks, up_blocks, gate_coords, gate_count,
             down_blocks, down_rows, down_coords, down_count):
        rows, width = tokens.shape
        n_model = width // BLOCK
        fb = FF // (BLOCK * n_gx)
        ca = (fb + 1) // 2
        cb = fb - ca
        cap, capd, used = gate_blocks.shape[2], down_blocks.shape[2], down_rows.shape[-1]
        hr = rows // halves
        rp = per * hr // n_gy
        jobs = nc * halves
        cfg = (n_gx, n_gy, n_hi, n_lo, per, nc, halves, rp, hr, n_model, fb, ca,
               cap, used, capd)
        wa, wb = ca * 2 * BLOCK, cb * 2 * BLOCK
        kl, kh, kg = max(n_lo - 1, 1), max(n_hi - 1, 1), max(n_gy - 1, 1)
        kp = max(per - 1, 1)
        tabs = -(-n_model * fb // LANES) + -(-used * n_model // LANES)
        vm, sm, dma = pltpu.VMEM, pltpu.SMEM, pltpu.SemaphoreType.DMA
        hbm = pl.BlockSpec(memory_space=pltpu.HBM)
        return pl.pallas_call(
            functools.partial(kernel, cfg),
            out_shape=pltpu.VMEM((rows, width), BF16),
            in_specs=[hbm] * 9,
            out_specs=pl.BlockSpec(memory_space=pltpu.VMEM),
            scratch_shapes=[
                sm((2, cap), I32),
                sm((1, 1), I32),
                sm((2, capd), I32),
                sm((1, 1), I32),
                sm(down_rows.shape, I32),
                vm((tabs, 1, LANES), I32),
                sm((tabs, 1, LANES), I32),
                vm((cap + 1, BLOCK, BLOCK), BF16),
                vm((cap + 1, BLOCK, BLOCK), BF16),
                vm((capd + 1, BLOCK, BLOCK), BF16),
                vm((nc, halves, per, hr, width), BF16),
                vm((jobs, n_hi, n_lo, rp, wa), BF16),
                vm((jobs, n_hi, n_lo, rp, wb), BF16),
                vm((jobs, kl, n_hi, rp, wa), BF16),
                vm((jobs, kh, n_lo, rp, wb), BF16),
                vm((jobs, kh, rp, wa), BF16),
                vm((jobs, kl, rp, wb), BF16),
                vm((jobs, kh, rp, wa), BF16),
                vm((jobs, kl, rp, wb), BF16),
                vm((jobs, rp, wa), F32),
                vm((jobs, rp, wb), F32),
                vm((fb, rp, BLOCK), BF16),
                vm((jobs, kg, rp, used * BLOCK), BF16),
                vm((jobs, n_gy, rp, used * BLOCK), BF16),
                vm((jobs, per * hr, width), BF16),
                vm((jobs, kp, hr, width), BF16),
                vm((jobs, hr, width), BF16),
                vm((nc, halves, hr, width), BF16),
                vm((halves, hr, width), F32),
                dma((8 + halves,)),
                dma((nc, halves, 2)), dma((kp,)), dma((nc, halves, per)),
                dma((1,)), dma((jobs,)),
                dma((1,)), dma((jobs,)),
                dma((1,)), dma((jobs,)),
                dma((1,)), dma((jobs,)),
                dma((1,)), dma((jobs,)),
                dma((1,)), dma((halves,)),
                dma((1,)), dma((jobs,)),
            ],
            compiler_params=pltpu.CompilerParams(
                collective_id=0, has_side_effects=True, vmem_limit_bytes=60 * 1024 * 1024),
        )(gate_coords[0, 0].T, gate_count, down_coords[0, 0].T, down_count, down_rows,
          tokens, gate_blocks.reshape(cap, BLOCK, BLOCK),
          up_blocks.reshape(cap, BLOCK, BLOCK), down_blocks.reshape(capd, BLOCK, BLOCK))

    return jax.shard_map(
        body,
        mesh=mesh,
        in_specs=(
            P("gx", "gy"),
            P("gy", "gx", None, None, None),
            P("gy", "gx", None, None, None),
            P("gy", "gx", None, None),
            P("gy", "gx"),
            P("gx", "gy", None, None, None),
            P("gx", None, None),
            P("gx", "gy", None, None),
            P("gx", "gy"),
        ),
        out_specs=P("gx", "gy"),
        check_vma=False,
    )
```

```python
import functools

import jax
import jax.numpy as jnp
from jax import lax
from jax.experimental import pallas as pl
from jax.experimental.pallas import tpu as pltpu
from jax.sharding import PartitionSpec as P

BLOCK = 128
LANES = 128
PIECES = 3
FF = 14336
MESH = pl.DeviceIdType.MESH
F32, BF16, I32 = jnp.float32, jnp.bfloat16, jnp.int32


def factor(n):
    low = 1
    while low * low * 4 <= n and n % (low * 2) == 0:
        low *= 2
    return n // low, low


def kernel(cfg, gco_h, gct_h, dco_h, dct_h, kept_h, tok, gblk, ublk, dblk, out,
           gco, gct, dco, dct, kept, tabv, tabs,
           gw, uw, dw, gat, pa, pb,
           r1a, r1b, s2a, s2b, r2a, r2b, acca, accb, hid, a2s, a2r, ps, fp, f2, fr, facc,
           lsem, gs, ks, gr, s1as, s1ar, s1bs, s1br, s2as, s2ar, s2bs, s2br, xs, xr, fs, fq, fps, fpr):
    (n_gx, n_gy, n_hi, n_lo, per, nc, halves, rp, hr, n_model, fb, ca,
     cap, used, capd) = cfg
    gx, gy = lax.axis_index("gx"), lax.axis_index("gy")
    zc, mc = gx // per, gx % per
    hi, lo = gy // n_lo, gy % n_lo
    tall = per * hr
    down_at = -(-n_model * fb // LANES)

    barrier = pltpu.get_barrier_semaphore()

    def greet(dev):
        pl.semaphore_signal(barrier, inc=1, device_id=dev, device_id_type=MESH)

    for d in range(1, n_lo):
        greet((gx, hi * n_lo + (lo + d) % n_lo))
    for d in range(1, n_hi):
        greet((gx, (hi + d) % n_hi * n_lo + lo))
    for d in range(1, per):
        greet((zc * per + (mc + d) % per, gy))

    @pl.when(zc > 0)
    def _():
        greet(((zc - 1) * per + mc, gy))

    @pl.when(zc < nc - 1)
    def _():
        greet(((zc + 1) * per + mc, gy))

    smalls = [
        pltpu.make_async_copy(gco_h, gco, lsem.at[0]),
        pltpu.make_async_copy(gct_h, gct, lsem.at[1]),
        pltpu.make_async_copy(dco_h, dco, lsem.at[2]),
        pltpu.make_async_copy(dct_h, dct, lsem.at[3]),
        pltpu.make_async_copy(kept_h, kept, lsem.at[4]),
    ]
    mine = [
        pltpu.make_async_copy(tok.at[pl.ds(h * hr, hr)], gat.at[zc, h, mc], lsem.at[8 + h])
        for h in range(halves)
    ]
    loads = [
        pltpu.make_async_copy(gblk, gw.at[pl.ds(0, cap)], lsem.at[5]),
        pltpu.make_async_copy(ublk, uw.at[pl.ds(0, cap)], lsem.at[6]),
        pltpu.make_async_copy(dblk, dw.at[pl.ds(0, capd)], lsem.at[7]),
    ]
    for load in smalls + mine + loads[:1]:
        load.start()

    def table(coords, count, slots, inner, spots, first):
        wide = -(-spots // LANES)
        lane = lax.broadcasted_iota(I32, (1, LANES), 1)
        row = [jnp.full((1, LANES), slots, I32) for _ in range(wide)]
        live = count[0, 0]
        for s in range(slots):
            place = coords[0, s] * inner + coords[1, s]
            place = jnp.where(s < live, place, -1)
            for w in range(wide):
                row[w] = jnp.where(lane + w * LANES == place, s, row[w])
        for w in range(wide):
            tabv[first + w] = row[w]

    with jax.named_scope("tables"):
        for load in smalls:
            load.wait()
        table(gco, gct, cap, fb, n_model * fb, 0)
        table(dco, dct, capd, n_model, used * n_model, down_at)
        gw[cap] = jnp.zeros((BLOCK, BLOCK), BF16)
        uw[cap] = jnp.zeros((BLOCK, BLOCK), BF16)
        dw[capd] = jnp.zeros((BLOCK, BLOCK), BF16)
        tables = pltpu.make_async_copy(tabv, tabs, lsem.at[0])
        tables.start()
        loads[1].start()
        for load in mine:
            load.wait()

    with jax.named_scope("barrier"):
        pl.semaphore_wait(
            barrier,
            n_lo + n_hi + per - 3 + jnp.minimum(zc, 1) + jnp.minimum(nc - 1 - zc, 1))

    sends = []

    def send(src, dst, ssem, rsem, dev, when=None, listed=False):
        copy = pltpu.make_async_remote_copy(
            src_ref=src, dst_ref=dst, send_sem=ssem, recv_sem=rsem,
            device_id=dev, device_id_type=MESH)
        if when is None:
            copy.start()
        else:
            pl.when(when)(copy.start)
        if listed:
            sends.append((copy, when))

    def left(ref, sem):
        pltpu.make_async_remote_copy(
            src_ref=ref, dst_ref=ref, send_sem=sem, recv_sem=sem,
            device_id=(gx, (gy + 1) % n_gy), device_id_type=MESH).wait_send()

    def arrived(ref, sem):
        with jax.named_scope("w"):
            pltpu.make_async_remote_copy(
                src_ref=ref, dst_ref=ref, send_sem=sem, recv_sem=sem,
                device_id=(gx, (gy + 1) % n_gy), device_id_type=MESH).wait_recv()

    def share(c, h, ways, there=None):
        ref = gat.at[c, h, mc]
        for at, way in enumerate(ways):
            to = zc + way
            fits = (to >= 0) & (to < nc)
            send(ref, ref, gs.at[nc if at else c, h], gr.at[c, h, mc], (to * per + mc, gy),
                 fits if there is None else there & fits, True)
        for j in range(1, per):
            send(ref, ref, ks.at[j - 1], gr.at[c, h, mc],
                 (zc * per + (mc + j) % per, gy), there)

    def relay(d, h, way):
        c = zc + way * d
        there = (c >= 0) & (c < nc)

        @pl.when(there)
        def _():
            arrived(gat.at[c, h, mc], gr.at[c, h, mc])

        share(c, h, (-way,), there)

    own = [(h, zc, h) for h in range(halves)]
    plain = [(k, h) for k in range(1, nc) for h in range(halves)]
    late = plain[:1] + [kh for kh in plain if kh[0] > 1] + plain[1:halves]
    peak = [(k, 0) for k in range(1, nc)] + [
        (k, h) for k in range(nc - 1, 0, -1) for h in range(1, halves)]

    def order(z):
        return peak if z == nc - 1 else plain if z % 2 else late

    top = 1 - jnp.minimum(nc - 1 - zc, 1)
    odd = zc % 2 * (1 - top)
    far = []
    for i, (a, b, c) in enumerate(zip(late, plain, peak)):
        k, h = (u + odd * (v - u) + top * (w - u) for u, v, w in zip(a, b, c))
        far.append((halves + i, zc ^ k, h))

    def spans(many, pieces):
        cut = many // 2
        ends = [0, 1, cut, many] if pieces > 1 and cut > 1 else [0, many]
        return list(zip(ends, ends[1:]))

    def project(first_job, count=1, pieces=1, between=None):
        j, chip, h = first_job
        for g in [h + i for i in range(count)]:
            for d in range(1, per):
                c = (mc + d) % per
                arrived(gat.at[chip, g, c], gr.at[chip, g, c])
        parts = ((pa, 0, ca), (pb, ca, fb - ca))
        for piece in range(pieces):
            for part, first, many in parts:
                cuts = spans(many, pieces)
                if piece >= len(cuts):
                    continue
                start, stop = cuts[piece]
                for t in range(start, stop):
                    columns = []
                    for b in (2 * t, 2 * t + 1):
                        ref, c = (gw, b) if b < many else (uw, b - many)
                        at = [r * fb + c + first for r in range(n_model)]
                        columns.append(jnp.concatenate(
                            [ref[tabs[a // LANES, 0, a % LANES]] for a in at], axis=0))
                    x = gat[chip, pl.ds(h, count)].reshape(count * tall, n_model * BLOCK)
                    y = jnp.dot(x, jnp.concatenate(columns, axis=1),
                                preferred_element_type=F32)
                    part[pl.ds(j, count), :, :, :, pl.ds(t * 2 * BLOCK, 2 * BLOCK)] = (
                        y.astype(BF16).reshape(count, n_hi, n_lo, rp, 2 * BLOCK))
                cols = pl.ds(start * 2 * BLOCK, (stop - start) * 2 * BLOCK)
                for g in range(j, j + count):
                    if part is pa:
                        for d in range(1, n_lo):
                            l2 = (lo + d) % n_lo
                            send(pa.at[g, :, l2, :, cols], r1a.at[g, d - 1, :, :, cols],
                                 s1as.at[0], s1ar.at[g],
                                 (gx, hi * n_lo + l2))
                    else:
                        for d in range(1, n_hi):
                            h2 = (hi + d) % n_hi
                            send(pb.at[g, h2, :, :, cols], r1b.at[g, d - 1, :, :, cols],
                                 s1bs.at[0], s1br.at[g],
                                 (gx, h2 * n_lo + lo))
            if between is not None and piece == max(pieces - 2, 0):
                between()

    def reduce(job):
        j = job[0]
        if n_lo > 1:
            arrived(r1a.at[j], s1ar.at[j])
        for e in list(range(1, n_hi)) + [0]:
            h2 = (hi + e) % n_hi
            s = pa[j, h2, lo].astype(F32)
            for d in range(1, n_lo):
                s = s + r1a[j, d - 1, h2].astype(F32)
            if e == 0:
                acca[j] = s
            else:
                s2a[j, e - 1] = s.astype(BF16)
                send(s2a.at[j, e - 1], r2a.at[j, e - 1], s2as.at[0], s2ar.at[j],
                     (gx, h2 * n_lo + lo))
        if n_hi > 1:
            arrived(r1b.at[j], s1br.at[j])
        for e in list(range(1, n_lo)) + [0]:
            l2 = (lo + e) % n_lo
            s = pb[j, hi, l2].astype(F32)
            for d in range(1, n_hi):
                s = s + r1b[j, d - 1, l2].astype(F32)
            if e == 0:
                accb[j] = s
            else:
                s2b[j, e - 1] = s.astype(BF16)
                send(s2b.at[j, e - 1], r2b.at[j, e - 1], s2bs.at[0], s2br.at[j],
                     (gx, hi * n_lo + l2))

    def activate(job):
        j = job[0]
        if n_hi > 1:
            arrived(r2a.at[j], s2ar.at[j])
        if n_lo > 1:
            arrived(r2b.at[j], s2br.at[j])
        for c in range(fb):
            acc, got, peers, at, many = (
                (acca, r2a, n_hi, c, ca) if c < ca else (accb, r2b, n_lo, c - ca, fb - ca))
            both = []
            for b in (at, many + at):
                cols = pl.ds(b * BLOCK, BLOCK)
                v = acc[j, :, cols]
                for d in range(1, peers):
                    v = v + got[j, d - 1, :, cols].astype(F32)
                both.append(v)
            gate, up = both
            hid[c] = (gate / (1.0 + jnp.exp(-gate)) * up).astype(BF16)
        others = [(a, b) for a in range(n_hi) for b in range(n_lo) if a or b]
        others.sort(key=lambda ab: -(ab[0] > 0) - (ab[1] > 0))
        for at, (a, b) in enumerate(others):
            dest = (hi + a) % n_hi * n_lo + (lo + b) % n_lo
            for q in range(used):
                a2s[j, at, :, pl.ds(q * BLOCK, BLOCK)] = hid[kept[0, dest, q]]
            send(a2s.at[j, at], a2r.at[j, gy], xs.at[0], xr.at[j], (gx, dest))
        for q in range(used):
            a2r[j, gy, :, pl.ds(q * BLOCK, BLOCK)] = hid[kept[0, gy, q]]

    wide = 2 * BLOCK

    def mix(job):
        j = job[0]
        if n_gy > 1:
            arrived(a2s.at[j], xr.at[j])

        def col(c, _):
            at = pl.multiple_of(c * wide, wide)
            slots = []
            for r in range(used):
                pair = [r * n_model + c * 2 + i for i in range(2)]
                slots.append([tabs[down_at + p // LANES, 0, p % LANES] for p in pair])
            weight = jnp.concatenate(
                [jnp.concatenate([dw[i] for i in pair], axis=1) for pair in slots], axis=0)
            ps[j, :, pl.ds(at, wide)] = jnp.dot(
                a2r[j].reshape(tall, used * BLOCK), weight,
                preferred_element_type=F32).astype(BF16)
            return 0

        lax.fori_loop(0, n_model * BLOCK // wide, col, 0, unroll=True)
        for d in range(1, per):
            cj = (mc + d) % per
            send(ps.at[j, pl.ds(pl.multiple_of(cj * hr, hr), hr)], fp.at[j, d - 1],
                 fps.at[0], fpr.at[j], (zc * per + cj, gy))

    def finish(job):
        j, chip, h = job
        s = ps[j, pl.ds(pl.multiple_of(mc * hr, hr), hr)].astype(F32)
        if per > 1:
            arrived(fp.at[j], fpr.at[j])
        for d in range(1, per):
            s = s + fp[j, d - 1].astype(F32)
        if j < halves:
            facc[j] = s
        else:
            f2[j] = s.astype(BF16)
            send(f2.at[j], fr.at[zc, h], fs.at[0], fq.at[h], (chip * per + mc, gy))

    def total(h):
        s = facc[h]
        if nc > 1:
            arrived(fr.at[pl.ds(0, nc - 1), h], fq.at[h])
        for k in range(1, nc):
            c = zc ^ k
            s = s + fr[c, h].astype(F32)
        out[pl.ds(h * hr, hr)] = s.astype(BF16)

    def run(stage, *args):
        tag = args[0][0] if isinstance(args[0], tuple) else args[0]
        with jax.named_scope(f"{stage.__name__}#j={tag}"):
            stage(*args)

    for h in range(halves):
        share(zc, h, (1, -1))
    tables.wait()
    with jax.named_scope("loads"):
        loads[0].wait()

    hops = {w: [(d, h) for d in range(1, nc) for h in range(halves)] for w in (-1, 1)}

    def need(i):
        for w in (-1, 1):
            reach = [(1, i)] if i < halves else []
            for z in range(nc if i < len(far) else 0):
                k, h = order(z)[i]
                if ((z ^ k) - z) * w > 0:
                    reach.append((abs((z ^ k) - z), h))
            while hops[w] and reach and hops[w][0] <= max(reach):
                run(relay, *hops[w].pop(0), w)

    n = len(far)

    def step(stage, i, *args):
        if 0 <= i < n:
            run(stage, far[i], *args)

    def more():
        loads[1].wait()
        loads[2].start()

    run(project, own[0], halves, PIECES, more)
    need(0)
    for i in range(n + 1):
        step(project, i, 1, PIECES)
        if i == 0:
            loads[2].wait()
            for w in (-1, 1):
                run(relay, *hops[w].pop(0), w)
            run(reduce, own[0])
            need(1)
        step(finish, i - 4)
        step(reduce, i - 1)
        step(activate, i - 2)
        if i == n:
            for job in own[1:]:
                run(reduce, job)
        step(mix, i - 3)
        if i:
            need(i + 1)
    step(activate, n - 1)
    run(activate, own[0])
    step(finish, n - 3)
    step(mix, n - 2)
    for job in own[1:]:
        run(activate, job)
    step(finish, n - 2)
    step(mix, n - 1)
    run(mix, own[0])
    step(finish, n - 1)
    for job in own[1:]:
        run(mix, job)
    for job in own:
        run(finish, job)
    for h in range(halves):
        run(total, h)
    for copy, when in sends:
        if when is None:
            copy.wait_send()
        else:
            pl.when(when)(copy.wait_send)
    for many, ref, sem in (
            (per, gat.at[:, :, 0], None), (n_lo, r1a, s1as), (n_hi, r1b, s1bs),
            (n_hi, s2a, s2as), (n_lo, s2b, s2bs), (n_gy, a2s, xs), (per, fp, fps),
            (nc, f2.at[pl.ds(halves, n)], fs)):
        if many > 1 and sem is not None:
            left(ref, sem.at[0])
        elif many > 1:
            for j in range(1, per):
                left(ref, ks.at[j - 1])


def solution(mesh):
    n_gx, n_gy = mesh.shape["gx"], mesh.shape["gy"]
    n_hi, n_lo = factor(n_gy)
    per = 2 if n_gx % 2 == 0 else 1
    nc = n_gx // per
    halves = 2

    def body(tokens, gate_blocks, up_blocks, gate_coords, gate_count,
             down_blocks, down_rows, down_coords, down_count):
        rows, width = tokens.shape
        n_model = width // BLOCK
        fb = FF // (BLOCK * n_gx)
        ca = (fb + 1) // 2
        cb = fb - ca
        cap, capd, used = gate_blocks.shape[2], down_blocks.shape[2], down_rows.shape[-1]
        hr = rows // halves
        rp = per * hr // n_gy
        jobs = nc * halves
        cfg = (n_gx, n_gy, n_hi, n_lo, per, nc, halves, rp, hr, n_model, fb, ca,
               cap, used, capd)
        wa, wb = ca * 2 * BLOCK, cb * 2 * BLOCK
        kl, kh, kg = max(n_lo - 1, 1), max(n_hi - 1, 1), max(n_gy - 1, 1)
        kp = max(per - 1, 1)
        tabs = -(-n_model * fb // LANES) + -(-used * n_model // LANES)
        vm, sm, dma = pltpu.VMEM, pltpu.SMEM, pltpu.SemaphoreType.DMA
        hbm = pl.BlockSpec(memory_space=pltpu.HBM)
        return pl.pallas_call(
            functools.partial(kernel, cfg),
            out_shape=pltpu.VMEM((rows, width), BF16),
            in_specs=[hbm] * 9,
            out_specs=pl.BlockSpec(memory_space=pltpu.VMEM),
            scratch_shapes=[
                sm((2, cap), I32),
                sm((1, 1), I32),
                sm((2, capd), I32),
                sm((1, 1), I32),
                sm(down_rows.shape, I32),
                vm((tabs, 1, LANES), I32),
                sm((tabs, 1, LANES), I32),
                vm((cap + 1, BLOCK, BLOCK), BF16),
                vm((cap + 1, BLOCK, BLOCK), BF16),
                vm((capd + 1, BLOCK, BLOCK), BF16),
                vm((nc, halves, per, hr, width), BF16),
                vm((jobs, n_hi, n_lo, rp, wa), BF16),
                vm((jobs, n_hi, n_lo, rp, wb), BF16),
                vm((jobs, kl, n_hi, rp, wa), BF16),
                vm((jobs, kh, n_lo, rp, wb), BF16),
                vm((jobs, kh, rp, wa), BF16),
                vm((jobs, kl, rp, wb), BF16),
                vm((jobs, kh, rp, wa), BF16),
                vm((jobs, kl, rp, wb), BF16),
                vm((jobs, rp, wa), F32),
                vm((jobs, rp, wb), F32),
                vm((fb, rp, BLOCK), BF16),
                vm((jobs, kg, rp, used * BLOCK), BF16),
                vm((jobs, n_gy, rp, used * BLOCK), BF16),
                vm((jobs, per * hr, width), BF16),
                vm((jobs, kp, hr, width), BF16),
                vm((jobs, hr, width), BF16),
                vm((nc, halves, hr, width), BF16),
                vm((halves, hr, width), F32),
                dma((8 + halves,)),
                dma((nc + 1, halves)), dma((kp,)), dma((nc, halves, per)),
                dma((1,)), dma((jobs,)),
                dma((1,)), dma((jobs,)),
                dma((1,)), dma((jobs,)),
                dma((1,)), dma((jobs,)),
                dma((1,)), dma((jobs,)),
                dma((1,)), dma((halves,)),
                dma((1,)), dma((jobs,)),
            ],
            compiler_params=pltpu.CompilerParams(
                collective_id=0, has_side_effects=True, vmem_limit_bytes=60 * 1024 * 1024),
        )(gate_coords[0, 0].T, gate_count, down_coords[0, 0].T, down_count, down_rows,
          tokens, gate_blocks.reshape(cap, BLOCK, BLOCK),
          up_blocks.reshape(cap, BLOCK, BLOCK), down_blocks.reshape(capd, BLOCK, BLOCK))

    return jax.shard_map(
        body,
        mesh=mesh,
        in_specs=(
            P("gx", "gy"),
            P("gy", "gx", None, None, None),
            P("gy", "gx", None, None, None),
            P("gy", "gx", None, None),
            P("gy", "gx"),
            P("gx", "gy", None, None, None),
            P("gx", None, None),
            P("gx", "gy", None, None),
            P("gx", "gy"),
        ),
        out_specs=P("gx", "gy"),
        check_vma=False,
    )
```
